512 devices in a mesh: gx: 8 (over z), gy: 8 (over y), gz: 8 (over x, core).
Axes of the slice: x: 4, y: 8, z: 8, core: 2. Of those that a mesh axis runs over, the one named last changes fastest.
Arguments:
- ref_pos: float32 [4096, 3, 128], P(('gx', 'gy', 'gz')), may hold values from -0.1 to 512, as said below
- displace: float32 [4096, 3, 128], P(('gx', 'gy', 'gz')), may hold values from -0.1 to 0.1
- velocity: float32 [4096, 3, 128], P(('gx', 'gy', 'gz')), may hold values from -15 to 15
- acceleration: float32 [4096, 3, 128], P(('gx', 'gy', 'gz')), may hold values from -6 to 6
- new_owner: int32 [4096], P(('gx', 'gy', 'gz')), may hold values from 0 to 511, as said below
- ghost_ids: int32 [12288], P(('gx', 'gy', 'gz')), may hold values from 0 to 4095, as said below
- pair_blocks: int32 [2, 110592], P(None, ('gx', 'gy', 'gz')), may hold values from 0 to 31, as said below
- pair_count: int32 [512], P(('gx', 'gy', 'gz')), may hold values from 1 to 216, as said below
- bond_bits: int32 [110592, 12, 128], P(('gx', 'gy', 'gz')), may hold values from 0 to 2047, as said below
Outputs:
- displace_new: float32 [4096, 3, 128], P(('gx', 'gy', 'gz'))
- velocity_new: float32 [4096, 3, 128], P(('gx', 'gy', 'gz'))
- acceleration_new: float32 [4096, 3, 128], P(('gx', 'gy', 'gz'))
The draws below stay inside these ranges and needn't reach their ends.
Inputs may be any that keep to these rules, and one draw needn't show every extreme that they name: `new_owner`: each block's new owner is its own device or one of the 26 devices around it in the grid gx by gy by gz, wrapping around every axis; exactly 2 blocks of each device get another owner, and every device is the new owner of exactly 8 blocks. `ghost_ids`: block indices in the new layout; each names a block whose new owner is one of the 26 devices around the device of the list, wrapping around; a list may name a block more than once; a list names at most 3 entries whose blocks have the same owner, and exactly 3 for some owner in every list. `pair_blocks`: row 0 is a slot of the device (below 8); row 1 is an index into the device's 8 blocks followed by its 24 ghost blocks. `pair_count`: at least one device has all 216 slots live in every draw. `bond_bits`: bits of particles at 128 or beyond are not used. `ref_pos`: reference positions of two different particles are at least 0.65 apart.
All inputs are finite; a program needn't handle non-finite values. Where the reference program divides by a largest or mean magnitude, that divisor is 1e-20 or more.
Results may differ from the reference program's by a relative error of at most 0.0003.
Values sent between devices are 32-bit elements; how exact they have to be, the bound alone decides.
No kernel may reach another device: no remote copies, remote signals or barrier semaphores. Data moves between devices by JAX's collectives and lax.ppermute only.
A program may use at most 64 MiB of HBM per device.

```python
import jax
import jax.numpy as jnp
import numpy as np
from jax import lax

BLOCK = 128
WORD_BITS = 11
BLK_DEV = 8
MOVE_MAX = 2
GHOSTS = 24
REQ_MAX = 3
PAIRS = 216
WORDS = 12
BLOCKS = 4096
N_GX = 8
N_GY = 8
N_GZ = 8
DEVICES = 512


def step_table():
    values = np.array([-1, 0, 1], dtype=np.int32)
    offsets_all = np.stack(np.meshgrid(values, values, values, indexing='ij'), axis=-1).reshape(27, 3)
    return np.concatenate([offsets_all[:13], offsets_all[14:]], axis=0)


def grid_place(device):
    return (device // (N_GY * N_GZ), device // N_GZ % N_GY, device % N_GZ)


def neighbour_of(device, steps):
    place_x, place_y, place_z = grid_place(device)
    moved_x = (place_x + steps[..., 0]) % N_GX
    moved_y = (place_y + steps[..., 1]) % N_GY
    moved_z = (place_z + steps[..., 2]) % N_GZ
    return (moved_x * N_GY + moved_y) * N_GZ + moved_z


def crack_plane(key):
    return jax.random.randint(jax.random.fold_in(key, 99), (), 0, N_GX, dtype=jnp.int32)


def skew_step(key, coords, axis_number, leading):
    extents = (N_GX, N_GY, N_GZ)
    others = [number for number in range(3) if number != axis_number]
    table_shape = (extents[others[0]], extents[others[1]])
    if leading:
        lookup = 2 * jax.random.randint(key, table_shape, 0, 2, dtype=jnp.int32) - 1
    else:
        lookup = jax.random.randint(key, table_shape, -1, 2, dtype=jnp.int32)
    offset_step = lookup[coords[others[0]], coords[others[1]]]
    shifted_coords = list(coords)
    shifted_coords[axis_number] = (coords[axis_number] + offset_step) % extents[axis_number]
    return shifted_coords


def skew_target(key, leading_axis, places):
    candidates = []
    for start_axis in range(3):
        coords = list(places)
        for section_number in range(3):
            section_key = jax.random.fold_in(key, start_axis * 3 + section_number)
            coords = skew_step(section_key, coords, (start_axis + section_number) % 3, section_number == 0)
        candidates.append((coords[0] * N_GY + coords[1]) * N_GZ + coords[2])
    stacked = jnp.stack(candidates, axis=0)
    return stacked[leading_axis]


def draw_new_owner(key, part):
    slot_key, route_key, lead_key = jax.random.split(jax.random.fold_in(key, 11), 3)
    devices = jnp.arange(DEVICES, dtype=jnp.int32)
    places = grid_place(devices)
    leads = jax.random.randint(lead_key, (MOVE_MAX,), 0, 3, dtype=jnp.int32)
    target_list = [skew_target(jax.random.fold_in(route_key, mover_index), leads[mover_index], places) for mover_index in range(MOVE_MAX)]
    targets = jnp.stack(target_list, axis=1).astype(jnp.int32)
    slot_keys = jax.random.split(slot_key, DEVICES)
    leaving = jax.vmap(lambda single: jax.random.permutation(single, BLK_DEV)[:MOVE_MAX])(slot_keys)
    owners = jnp.broadcast_to(devices[:, None], (DEVICES, BLK_DEV))
    owners = owners.at[devices[:, None], leaving].set(targets)
    return owners.reshape(-1).astype(jnp.int32)


def draw_ghost_ids(key, part):
    order_key, slot_key, place_key = jax.random.split(jax.random.fold_in(key, 12), 3)
    steps_np = step_table()
    sizes_np = np.array([N_GX, N_GY, N_GZ], dtype=np.int32)
    barred = jnp.asarray(np.any((steps_np == -1) & (sizes_np[None, :] == 2), axis=1).astype(np.int32))
    step_rows = jnp.asarray(steps_np)
    devices = jnp.arange(DEVICES, dtype=jnp.int32)

    def choose(single):
        order = jax.random.permutation(single, 26).astype(jnp.int32)
        return order[jnp.argsort(barred[order], stable=True)]
    chosen = jax.vmap(choose)(jax.random.split(order_key, DEVICES))
    spread = jax.vmap(lambda single: jax.random.permutation(single, GHOSTS))(jax.random.split(place_key, DEVICES)).astype(jnp.int32)
    picked = jnp.take_along_axis(chosen, spread // REQ_MAX, axis=1)
    slot_ids = jax.random.randint(slot_key, (DEVICES, GHOSTS), 0, BLK_DEV, dtype=jnp.int32)
    owners = neighbour_of(devices[:, None], step_rows[picked])
    return (owners * BLK_DEV + slot_ids).reshape(-1).astype(jnp.int32)


def draw_pair_count(key, part):
    devices = jnp.arange(DEVICES, dtype=jnp.int32)
    modest = jax.random.randint(jax.random.fold_in(key, 13), (DEVICES,), PAIRS // 8 + 1, PAIRS // 3 + 1, dtype=jnp.int32)
    return jnp.where(devices // (N_GY * N_GZ) == crack_plane(key), PAIRS, modest).astype(jnp.int32)


def draw_pair_blocks(key, part):
    home_key, away_key = jax.random.split(jax.random.fold_in(key, 14))
    home_ids = jax.random.randint(home_key, (DEVICES * PAIRS,), 0, BLK_DEV, dtype=jnp.int32)
    away_ids = jax.random.randint(away_key, (DEVICES * PAIRS,), 0, BLK_DEV + GHOSTS, dtype=jnp.int32)
    return jnp.stack([home_ids, away_ids], axis=0)


def draw_bond_bits(key, part):
    full_shape = (DEVICES * PAIRS, WORDS, BLOCK)
    key_list = jax.random.split(jax.random.fold_in(key, 15), 7)
    ceiling = 2 ** WORD_BITS
    merged = jax.random.randint(key_list[0], full_shape, 0, ceiling, dtype=jnp.int32)
    for number in range(1, 5):
        merged = jnp.bitwise_and(merged, jax.random.randint(key_list[number], full_shape, 0, ceiling, dtype=jnp.int32))
    further = jnp.bitwise_and(jax.random.randint(key_list[5], full_shape, 0, ceiling, dtype=jnp.int32), jax.random.randint(key_list[6], full_shape, 0, ceiling, dtype=jnp.int32))
    device_x = jnp.arange(DEVICES * PAIRS, dtype=jnp.int32) // PAIRS // (N_GY * N_GZ)
    cracked = (device_x == crack_plane(key))[:, None, None]
    return jnp.where(cracked, jnp.bitwise_and(merged, further), merged).astype(jnp.int32)


def draw_ref_pos(key, part):
    lattice_key = jax.random.fold_in(jax.random.fold_in(key, 16), 0)
    index_b = jnp.arange(BLOCKS, dtype=jnp.int32)
    device = index_b // BLK_DEV
    inside = index_b % BLK_DEV
    place_x, place_y, place_z = grid_place(device)
    length_x = BLOCK // 16
    member = jnp.arange(BLOCK, dtype=jnp.int32)
    corner_x = (place_x * BLK_DEV + inside) * length_x
    coord_x = corner_x[:, None] + member[None, :] // 16
    coord_y = (place_y * 4)[:, None] + member[None, :] // 4 % 4
    coord_z = (place_z * 4)[:, None] + member[None, :] % 4
    lattice = jnp.stack([coord_x, coord_y, coord_z], axis=1).astype(jnp.float32)
    jitter = jax.random.uniform(lattice_key, (BLOCKS, 3, BLOCK), jnp.float32, -0.1, 0.1)
    return lattice + jitter


def draw_velocity(key, part):
    drawn_key = jax.random.fold_in(key, 17)
    full_shape = (BLOCKS, 3, BLOCK)
    drawn = jnp.clip(jax.random.normal(drawn_key, full_shape, jnp.float32), -5.0, 5.0)
    rising = 1.0 + 2.0 * jnp.arange(BLOCKS, dtype=jnp.float32) / (BLOCKS - 1)
    return drawn * rising[:, None, None]


def block_levels(stream_key, dims, cuts, low, top_value):
    factor_of, own = 1.0, jax.random.fold_in(stream_key, 6)
    for dim, blocks in cuts:
        steps = jnp.exp(jax.random.uniform(jax.random.fold_in(own, dim), (blocks,), jnp.float32, low / len(cuts), top_value / len(cuts)))
        factor_of = factor_of * jnp.repeat(steps, dims[dim] // blocks).reshape([-1 if axis == dim else 1 for axis in range(len(dims))])
    return factor_of


def gaussian(key, shape, scale, limit, cuts=(), kind=jnp.bfloat16):
    entries = scale * jax.random.normal(key, shape, jnp.float32)
    if cuts:
        entries = entries * block_levels(key, shape, cuts, -0.22, 0.18)
    return jnp.clip(entries, -limit, limit).astype(kind)


def setup_inputs(seed: int = 0) -> dict:
    seeds = jax.random.split(jax.random.key(seed), 10)
    ref_pos = draw_ref_pos(jax.random.fold_in(seeds[9], 71), 0)
    displace = jnp.clip(jax.random.uniform(seeds[1], (BLOCKS, 3, BLOCK), jnp.float32, -0.1, 0.1) * block_levels(seeds[1], (BLOCKS, 3, BLOCK), ((0, 512),), -0.4, 0.0), -0.1, 0.1)
    velocity = draw_velocity(jax.random.fold_in(seeds[9], 71), 0)
    acceleration = gaussian(seeds[3], (BLOCKS, 3, BLOCK), 1.0, 6.0, ((0, 512),), jnp.float32)
    new_owner = draw_new_owner(jax.random.fold_in(seeds[9], 71), 0)
    ghost_ids = draw_ghost_ids(jax.random.fold_in(seeds[9], 71), 0)
    pair_blocks = draw_pair_blocks(jax.random.fold_in(seeds[9], 71), 0)
    pair_count = draw_pair_count(jax.random.fold_in(seeds[9], 71), 0)
    bond_bits = draw_bond_bits(jax.random.fold_in(seeds[9], 71), 0)
    return {"ref_pos": ref_pos, "displace": displace, "velocity": velocity, "acceleration": acceleration, "new_owner": new_owner, "ghost_ids": ghost_ids, "pair_blocks": pair_blocks, "pair_count": pair_count, "bond_bits": bond_bits}


courant = 0.05
stiffness = 20.0

def tile_force(home_tile, away_tile, same_block, bit_words, live_mask):
    particles = home_tile.shape[2]
    ref_gap = away_tile[:, 0:3, :, None] - home_tile[:, 0:3, None, :]
    now_gap = ref_gap + (away_tile[:, 3:6, :, None] - home_tile[:, 3:6, None, :])
    rest_len = jnp.sqrt(lax.optimization_barrier(jnp.sum(ref_gap * ref_gap, axis=1)))
    now_len = jnp.sqrt(lax.optimization_barrier(jnp.sum(now_gap * now_gap, axis=1)))
    column = jnp.arange(particles).astype(jnp.int32)
    word_rows = jnp.take(bit_words, column // WORD_BITS, axis=1)
    intact = jnp.bitwise_and(jnp.right_shift(word_rows, (column % WORD_BITS)[None, :, None]), 1)
    selfish = same_block[:, None, None] & (column[:, None] == column[None, :])[None, :, :]
    weight = jnp.where(selfish, 0.0, intact.astype(jnp.float32)) * live_mask[:, None, None]
    safe_len = jnp.where(selfish, 1.0, rest_len)
    safe_now = jnp.where(selfish, 1.0, now_len)
    scaled = weight * ((now_len - rest_len) / safe_len) / safe_now
    return lax.optimization_barrier(jnp.sum(scaled[:, None, :, :] * now_gap, axis=2))

def reference(ref_pos, displace, velocity, acceleration, new_owner, ghost_ids, pair_blocks, pair_count, bond_bits):
    fastest = jnp.max(jnp.abs(velocity))
    timestep = courant / (fastest + 1e-06)
    halfway = velocity + 0.5 * timestep * acceleration
    shifted = displace + timestep * halfway
    ordering = jnp.argsort(new_owner, stable=True)
    ref_new = ref_pos[ordering]
    shifted_new = shifted[ordering]
    halfway_new = halfway[ordering]
    local_all = jnp.concatenate([ref_new, shifted_new], axis=1)
    particles = ref_pos.shape[2]
    locals_dev = local_all.reshape(DEVICES, BLK_DEV, 6, particles)
    ghosts_dev = local_all[ghost_ids].reshape(DEVICES, GHOSTS, 6, particles)
    homes = pair_blocks[0].reshape(DEVICES, PAIRS)
    aways = pair_blocks[1].reshape(DEVICES, PAIRS)
    bit_dev = bond_bits.reshape(DEVICES, PAIRS, WORDS, particles)

    def per_device(packed):
        local_set, ghost_set, home_ids, away_ids, bit_words, live_count = packed
        extended = jnp.concatenate([local_set, ghost_set], axis=0)
        live_mask = (jnp.arange(PAIRS).astype(jnp.int32) < live_count).astype(jnp.float32)
        tile_sum = tile_force(local_set[home_ids], extended[away_ids], home_ids == away_ids, bit_words, live_mask)
        return jnp.zeros((BLK_DEV, 3, particles), jnp.float32).at[home_ids].add(tile_sum)
    bond_sum = lax.map(per_device, (locals_dev, ghosts_dev, homes, aways, bit_dev, pair_count))
    acceleration_new = stiffness * bond_sum.reshape(BLOCKS, 3, particles)
    velocity_new = halfway_new + 0.5 * timestep * acceleration_new
    return (shifted_new, velocity_new, acceleration_new)
```

```python
import jax
import jax.numpy as jnp
import numpy as np
from jax import lax
from jax.experimental import pallas as pl
from jax.experimental.pallas import tpu as pltpu
from jax.sharding import PartitionSpec as P

WORD_BITS = 11
AXES = ("gx", "gy", "gz")

courant = 0.05
stiffness = 20.0


MOVE = 2
COMPS = 12
PACK = 32
CELL = 104


def particle_order(words):
    order = []
    for bit in range(WORD_BITS):
        order += [WORD_BITS * row + bit for row in range(8)]
    for bit in range(5):
        order += [WORD_BITS * (8 + row) + bit for row in range(3)]
        order += [WORD_BITS * 11 + bit]
        order += [WORD_BITS * (8 + row) + 5 + bit for row in range(3)]
        order += [WORD_BITS * 11 + 5 + bit if bit < 2 else WORD_BITS * (6 + bit) + 10]
    return np.array(order, np.int32)


def self_bits(order):
    lost = np.zeros((16, 128), np.int32)
    for place, particle in enumerate(order):
        vector, row = place // 8, place % 8
        if vector < WORD_BITS:
            lost[row, particle] |= 1 << vector
        else:
            lost[8 + row, particle] |= 1 << (vector - WORD_BITS)
    return ~lost


def pack_kernel(owner_ref, self_ref, ref_ref, dis_ref, vel_ref, acc_ref, out_ref):
    myself = self_ref[0]
    first = jnp.int32(0)
    second = jnp.int32(0)
    found = jnp.bool_(False)
    for k in range(8):
        leaves = owner_ref[k] != myself
        first = jnp.where(leaves & jnp.logical_not(found), k, first)
        second = jnp.where(leaves & found, k, second)
        found = found | leaves
    for group, source in enumerate((ref_ref, dis_ref, vel_ref, acc_ref)):
        for c in range(3):
            out_ref[pl.ds(group * 3 + c, 1), :] = source[c, pl.ds(first, 1), :]
            out_ref[pl.ds(12 + group * 3 + c, 1), :] = source[c, pl.ds(second, 1), :]
    lane = lax.broadcasted_iota(jnp.int32, (8, 128), 1)
    values = (
        owner_ref[first],
        owner_ref[second],
        myself * 8 + first,
        myself * 8 + second,
    )
    misc = jnp.zeros((8, 128), jnp.float32)
    for place, value in enumerate(values):
        misc = jnp.where(lane == place, value.astype(jnp.float32), misc)
    out_ref[24:32, :] = misc
    speed = jnp.maximum(
        jnp.maximum(jnp.abs(vel_ref[0]), jnp.abs(vel_ref[1])), jnp.abs(vel_ref[2])
    )
    out_ref[32:40, :] = jnp.full((8, 128), jnp.max(speed), jnp.float32)


def settle_kernel(pick_ref, ref_ref, dis_ref, vel_ref, acc_ref, cand_ref, top_ref, out_ref):
    for k in range(8):
        pick = pick_ref[k]
        own = pick < 8
        place = jnp.where(own, pick, 0)
        moved = jnp.where(own, 0, pick - 8)
        base = (moved // MOVE) * PACK + (moved % MOVE) * COMPS
        for group, source in enumerate((ref_ref, dis_ref, vel_ref, acc_ref)):
            for c in range(3):
                row = group * 3 + c
                kept = source[c, pl.ds(place, 1), :]
                come = cand_ref[pl.ds(base + row, 1), :]
                out_ref[pl.ds(row * 8 + k, 1), :] = jnp.where(own, kept, come)
    out_ref[96:104, :] = top_ref[...]


def force_kernel(
    pair_ref,
    count_ref,
    source_ref,
    around_ref,
    bits_ref,
    tail_ref,
    keep_ref,
    lane_ref,
    dis_ref,
    vel_ref,
    acc_ref,
    raw_ref,
    ext_ref,
    table_ref,
    sums_ref,
):
    pairs = pair_ref.shape[1]
    fastest = around_ref[96:104, :]
    for cell in range(1, 27):
        fastest = jnp.maximum(fastest, around_ref[cell * CELL + 96 : cell * CELL + 104, :])
    timestep = courant / (fastest + 1e-06)
    half_step = 0.5 * timestep

    def own(c):
        start = 13 * CELL + 8 * c
        return around_ref[start : start + 8, :]

    for c in range(3):
        halfway = own(6 + c) + half_step * own(9 + c)
        shifted = own(3 + c) + timestep * halfway
        dis_ref[c] = shifted
        vel_ref[c] = halfway
        ext_ref[c * 32 : c * 32 + 8, :] = own(c)
        ext_ref[(3 + c) * 32 : (3 + c) * 32 + 8, :] = shifted

    for g in range(24):
        start = source_ref[g]
        for c in range(COMPS):
            raw_ref[c * 24 + g : c * 24 + g + 1, :] = around_ref[pl.ds(start + 8 * c, 1), :]

    for c in range(3):
        for t in range(3):

            def raw(n):
                return raw_ref[n * 24 + t * 8 : n * 24 + t * 8 + 8, :]

            halfway = raw(6 + c) + half_step * raw(9 + c)
            row = 8 + t * 8
            ext_ref[c * 32 + row : c * 32 + row + 8, :] = raw(c)
            ext_ref[(3 + c) * 32 + row : (3 + c) * 32 + row + 8, :] = raw(3 + c) + timestep * halfway

    lanes = lane_ref[...]

    def spread(i, carry):
        tile = ext_ref[pl.ds(pl.multiple_of(i * 8, 8), 8), :]
        tile = jnp.take_along_axis(tile, lanes, axis=1, mode="promise_in_bounds")
        for r in range(8):
            table_ref[i * 8 + r] = jnp.broadcast_to(tile[r : r + 1, :], (128, 128)).T
        return carry

    lax.fori_loop(0, 24, spread, 0)

    for k in range(24):
        sums_ref[k] = jnp.zeros((8, 128), jnp.float32)

    count = count_ref[0]
    keep_head = keep_ref[0:8, :]
    keep_tail = keep_ref[8:16, :]

    def one_pair(p):
        home = pair_ref[0, p]
        away = pair_ref[1, p]
        everything = jnp.where(home == away, 0, -1)
        live = jnp.where(p < count, -1, 0)
        head = bits_ref[pl.ds(p, 8, stride=pairs), :] & (keep_head | everything) & live
        tail = tail_ref[pl.ds(p, 8, stride=pairs), :] & (keep_tail | everything) & live
        here = [
            jnp.broadcast_to(ext_ref[pl.ds(c * 32 + home, 1), :], (8, 128)) for c in range(6)
        ]
        force = [jnp.zeros((8, 128), jnp.float32) for _ in range(3)]
        for v in range(16):
            word, bit = (head, 1 << v) if v < WORD_BITS else (tail, 1 << (v - WORD_BITS))
            there = [table_ref[c * 32 + away, v * 8 : v * 8 + 8, :] for c in range(6)]
            gap = [there[c] - here[c] for c in range(3)]
            now = [gap[c] + (there[3 + c] - here[3 + c]) for c in range(3)]
            rest2 = gap[0] * gap[0] + gap[1] * gap[1] + gap[2] * gap[2]
            now2 = now[0] * now[0] + now[1] * now[1] + now[2] * now[2]
            scaled = lax.rsqrt(rest2) - lax.rsqrt(now2)
            scaled = jnp.where((word & bit) != 0, scaled, 0.0)
            force = [force[c] + scaled * now[c] for c in range(3)]
        for c in range(3):
            sums_ref[home * 3 + c] += force[c]

    def step(q, carry):
        one_pair(2 * q)
        one_pair(2 * q + 1)
        return carry

    lax.fori_loop(0, (count + 1) // 2, step, 0)

    for c in range(3):
        rows = [jnp.sum(sums_ref[h * 3 + c], axis=0, keepdims=True) for h in range(8)]
        acceleration = stiffness * jnp.concatenate(rows, axis=0)
        acc_ref[c] = acceleration
        vel_ref[c] = vel_ref[c] + half_step * acceleration


def call_pack(owner, myself, fields):
    smem = pl.BlockSpec(memory_space=pltpu.SMEM)
    vmem = pl.BlockSpec(memory_space=pltpu.VMEM)
    return pl.pallas_call(
        pack_kernel,
        out_shape=jax.ShapeDtypeStruct((40, 128), jnp.float32),
        in_specs=[smem, smem] + [vmem] * 4,
        out_specs=vmem,
        name="pack",
    )(owner, myself, *fields)


def call_settle(picks, fields, candidates, top):
    smem = pl.BlockSpec(memory_space=pltpu.SMEM)
    vmem = pl.BlockSpec(memory_space=pltpu.VMEM)
    return pl.pallas_call(
        settle_kernel,
        out_shape=jax.ShapeDtypeStruct((CELL, 128), jnp.float32),
        in_specs=[smem] + [vmem] * 6,
        out_specs=vmem,
        name="settle",
    )(picks, *fields, candidates, top)


def call_force(pair_blocks, pair_count, sources, around, bond_bits):
    smem = pl.BlockSpec(memory_space=pltpu.SMEM)
    vmem = pl.BlockSpec(memory_space=pltpu.VMEM)
    pairs = pair_blocks.shape[1]
    words = jnp.transpose(bond_bits, (1, 0, 2))
    low = jnp.bitwise_and(words[8:12], 31)
    high = jnp.right_shift(words[8:12], 5)
    last = jnp.bitwise_and(high[3:4], 3)
    for n in range(3):
        last = last | ((high[n : n + 1] >> 5) & 1) << (2 + n)
    tail = jnp.concatenate([low, jnp.bitwise_and(high[0:3], 31), last], axis=0)
    order = particle_order(12)
    keep = jnp.asarray(self_bits(order))
    lanes = jnp.asarray(np.broadcast_to(order[None, :], (8, 128)).copy())
    tile = jax.ShapeDtypeStruct((3, 8, 128), jnp.float32)
    return pl.pallas_call(
        force_kernel,
        out_shape=(tile, tile, tile),
        in_specs=[smem, smem, smem] + [vmem] * 5,
        out_specs=(vmem, vmem, vmem),
        scratch_shapes=[
            pltpu.VMEM((COMPS * 24, 128), jnp.float32),
            pltpu.VMEM((6 * 32, 128), jnp.float32),
            pltpu.VMEM((6 * 32, 128, 128), jnp.float32),
            pltpu.VMEM((24, 8, 128), jnp.float32),
        ],
        compiler_params=pltpu.CompilerParams(vmem_limit_bytes=40 * 1024 * 1024),
        name="forces",
    )(
        pair_blocks,
        pair_count,
        sources,
        around,
        words.reshape(12 * pairs, 128),
        tail.reshape(8 * pairs, 128),
        keep,
        lanes,
    )


def shifted_by(shard, axis, amount):
    size = lax.axis_size(axis)
    return lax.ppermute(shard, axis, [(i, (i + amount) % size) for i in range(size)])


def around_index(offset, extent):
    wrapped = offset % extent
    return jnp.where(wrapped == 0, 1, jnp.where(wrapped == 1, 2, 0))


def choose(owner, myself, candidates, blocks):
    misc = candidates.reshape(27, PACK, 128)[:, 24, 0:4].astype(jnp.int32)
    own_ids = myself * blocks + jnp.arange(blocks, dtype=jnp.int32)
    owners = jnp.concatenate([owner, misc[:, 0:2].reshape(-1)])
    labels = jnp.concatenate([own_ids, misc[:, 2:4].reshape(-1)])
    chosen = owners == myself
    before = chosen[None, :] & (labels[None, :] < labels[:, None])
    ranked = jnp.sum(before.astype(jnp.int32), axis=1)
    places = jnp.arange(blocks, dtype=jnp.int32)
    matches = chosen[None, :] & (ranked[None, :] == places[:, None])
    numbers = jnp.arange(owners.shape[0], dtype=jnp.int32)
    return jnp.sum(jnp.where(matches, numbers[None, :], 0), axis=1)


def per_device(
    ref_pos,
    displace,
    velocity,
    acceleration,
    new_owner,
    ghost_ids,
    pair_blocks,
    pair_count,
    bond_bits,
):
    blocks = ref_pos.shape[0]
    size_x, size_y, size_z = (lax.axis_size(axis) for axis in AXES)
    place_x, place_y, place_z = (lax.axis_index(axis) for axis in AXES)
    myself = ((place_x * size_y + place_y) * size_z + place_z).astype(jnp.int32)
    fields = tuple(
        jnp.transpose(field, (1, 0, 2)) for field in (ref_pos, displace, velocity, acceleration)
    )

    packed = call_pack(new_owner, myself[None], fields)
    body, top = packed[:PACK], packed[PACK:]
    for axis in AXES:
        whole = jnp.concatenate([body, top], axis=0)
        before = shifted_by(whole, axis, 1)
        after = shifted_by(whole, axis, -1)
        across = shifted_by(top, axis, 4)
        top = jnp.maximum(jnp.maximum(top, across), jnp.maximum(before[-8:], after[-8:]))
        body = jnp.concatenate([before[:-8], body, after[:-8]], axis=0)
    picks = choose(new_owner, myself, body, blocks)
    around = call_settle(picks, fields, body, top)

    ghost_dev = ghost_ids // blocks
    ghost_slot = ghost_ids % blocks
    ghost_cell = (
        around_index(ghost_dev // (size_y * size_z) - place_x, size_x)
        + around_index(ghost_dev // size_z % size_y - place_y, size_y) * 3
        + around_index(ghost_dev % size_z - place_z, size_z) * 9
    )
    sources = (ghost_cell * CELL + ghost_slot).astype(jnp.int32)
    for axis in AXES:
        before = shifted_by(around, axis, 1)
        after = shifted_by(around, axis, -1)
        around = jnp.concatenate([before, around, after], axis=0)
    outs = call_force(pair_blocks, pair_count, sources, around, bond_bits)
    return tuple(jnp.transpose(out, (1, 0, 2)) for out in outs)


def solution(mesh):
    wide = P(AXES, None, None)
    in_specs = (wide,) * 4 + (P(AXES), P(AXES), P(None, AXES), P(AXES), wide)
    return jax.shard_map(
        per_device, mesh=mesh, in_specs=in_specs, out_specs=(wide,) * 3, check_vma=False
    )
```

```python
import jax
import jax.numpy as jnp
import numpy as np
from jax import lax
from jax.experimental import pallas as pl
from jax.experimental.pallas import tpu as pltpu
from jax.sharding import PartitionSpec as P

WORD_BITS = 11
AXES = ("gx", "gy", "gz")

courant = 0.05
stiffness = 20.0


MOVE = 2
COMPS = 12
PACK = 32
CELL = 104
LINE = 3 * CELL + 8
PLANE = 3 * LINE + 8
GROUP = 8
STEADY = 3


LANE_GATHER = lax.GatherDimensionNumbers(
    offset_dims=(),
    collapsed_slice_dims=(1,),
    start_index_map=(1,),
    operand_batching_dims=(0,),
    start_indices_batching_dims=(0,),
)


def by_lane(table, particle):
    return lax.gather(
        table,
        particle[:, :, None],
        LANE_GATHER,
        slice_sizes=(1, 1),
        mode=lax.GatherScatterMode.PROMISE_IN_BOUNDS,
    )


def prepare_kernel(words_ref, wide_ref, most_ref):
    pairs = words_ref.shape[1]

    def group(g, carry):
        start = pl.multiple_of(g * GROUP, GROUP)
        words = [words_ref[w, pl.ds(start, GROUP), :] for w in range(12)]
        most = None
        for t in range(4):
            total = None
            for w in range(12):
                move = WORD_BITS * w - 32 * t
                if -WORD_BITS < move < 32:
                    part = words[w] << move if move >= 0 else words[w] >> -move
                    total = part if total is None else total | part
            wide_ref[t, pl.ds(start, GROUP), :] = total
            wide_ref[4 + t, pl.ds(start, GROUP), :] = total
            used = lax.population_count(total)
            most = used if most is None else jnp.maximum(most, used)
        most_ref[pl.ds(g, 1), :] = jnp.max(most, axis=0, keepdims=True)
        return carry

    lax.fori_loop(0, pairs // GROUP, group, 0)


def call_prepare(bond_bits):
    pairs = bond_bits.shape[0]
    vmem = pl.BlockSpec(memory_space=pltpu.VMEM)
    wide, most = pl.pallas_call(
        prepare_kernel,
        out_shape=(
            jax.ShapeDtypeStruct((8, pairs, 128), jnp.int32),
            jax.ShapeDtypeStruct((pairs // GROUP, 128), jnp.int32),
        ),
        in_specs=[vmem],
        out_specs=(vmem, vmem),
        cost_estimate=pl.CostEstimate(
            flops=20_000_000, bytes_accessed=2_200_000, transcendentals=0
        ),
        name="prepare",
    )(jnp.transpose(bond_bits, (1, 0, 2)))
    return wide.reshape(8 * pairs, 128), jnp.max(most, axis=1)


def self_bits():
    bit = np.arange(128)[None, :] - 32 * (np.arange(8)[:, None] % 4)
    lost = np.where((bit >= 0) & (bit < 32), np.int64(1) << np.clip(bit, 0, 31), 0)
    return (~lost).astype(np.uint32).view(np.int32)


def pack_kernel(owner_ref, self_ref, ref_ref, dis_ref, vel_ref, acc_ref, out_ref):
    myself = self_ref[0]
    first = jnp.int32(0)
    second = jnp.int32(0)
    found = jnp.bool_(False)
    for k in range(8):
        leaves = owner_ref[k] != myself
        first = jnp.where(leaves & jnp.logical_not(found), k, first)
        second = jnp.where(leaves & found, k, second)
        found = found | leaves
    for group, source in enumerate((ref_ref, dis_ref, vel_ref, acc_ref)):
        for c in range(3):
            out_ref[pl.ds(group * 3 + c, 1), :] = source[c, pl.ds(first, 1), :]
            out_ref[pl.ds(12 + group * 3 + c, 1), :] = source[c, pl.ds(second, 1), :]
    lane = lax.broadcasted_iota(jnp.int32, (8, 128), 1)
    values = (
        owner_ref[first],
        owner_ref[second],
        myself * 8 + first,
        myself * 8 + second,
    )
    misc = jnp.zeros((8, 128), jnp.float32)
    for place, value in enumerate(values):
        misc = jnp.where(lane == place, value.astype(jnp.float32), misc)
    speed = jnp.maximum(
        jnp.maximum(jnp.abs(vel_ref[0]), jnp.abs(vel_ref[1])), jnp.abs(vel_ref[2])
    )
    row = lax.broadcasted_iota(jnp.int32, (8, 128), 0)
    out_ref[24:32, :] = jnp.where(row == 0, misc, jnp.max(speed))


def settle_kernel(pick_ref, ref_ref, dis_ref, vel_ref, acc_ref, cand_ref, out_ref, top_ref):
    for k in range(8):
        pick = pick_ref[k]
        own = pick < 8
        place = jnp.where(own, pick, 0)
        moved = jnp.where(own, 0, pick - 8)
        base = (moved // MOVE) * PACK + (moved % MOVE) * COMPS
        for group, source in enumerate((ref_ref, dis_ref, vel_ref, acc_ref)):
            for c in range(3):
                row = group * 3 + c
                kept = source[c, pl.ds(place, 1), :]
                come = cand_ref[pl.ds(base + row, 1), :]
                out_ref[pl.ds(row * 8 + k, 1), :] = jnp.where(own, kept, come)
    top = cand_ref[25:26, :]
    for cell in range(1, 27):
        top = jnp.maximum(top, cand_ref[cell * PACK + 25 : cell * PACK + 26, :])
    top = jnp.broadcast_to(top, (8, 128))
    out_ref[96:104, :] = top
    top_ref[...] = top


def force_kernel(
    pair_ref,
    count_ref,
    source_ref,
    rounds_ref,
    around_ref,
    far_ref,
    bits_ref,
    keep_ref,
    dis_ref,
    vel_ref,
    acc_ref,
    raw_ref,
    ext_ref,
    left_ref,
    sums0_ref,
    sums1_ref,
    sums2_ref,
    sums3_ref,
):
    pairs = pair_ref.shape[1]
    fastest = far_ref[...]
    for z in range(3):
        tops = [PLANE * z + 3 * LINE]
        for y in range(3):
            start = PLANE * z + LINE * y
            tops += [start + 96, start + CELL + 96, start + 2 * CELL + 96, start + 3 * CELL]
        for start in tops:
            fastest = jnp.maximum(fastest, around_ref[start : start + 8, :])
    timestep = courant / (fastest + 1e-06)
    half_step = 0.5 * timestep

    def own(c):
        start = PLANE + LINE + CELL + 8 * c
        return around_ref[start : start + 8, :]

    for c in range(3):
        halfway = own(6 + c) + half_step * own(9 + c)
        shifted = own(3 + c) + timestep * halfway
        dis_ref[c] = shifted
        vel_ref[c] = halfway
        ext_ref[c * 32 : c * 32 + 8, :] = own(c)
        ext_ref[(3 + c) * 32 : (3 + c) * 32 + 8, :] = shifted

    for g in range(24):
        start = source_ref[g]
        for c in range(COMPS):
            raw_ref[c * 24 + g : c * 24 + g + 1, :] = around_ref[pl.ds(start + 8 * c, 1), :]

    for c in range(3):
        for t in range(3):

            def raw(n):
                return raw_ref[n * 24 + t * 8 : n * 24 + t * 8 + 8, :]

            halfway = raw(6 + c) + half_step * raw(9 + c)
            row = 8 + t * 8
            ext_ref[c * 32 + row : c * 32 + row + 8, :] = raw(c)
            ext_ref[(3 + c) * 32 + row : (3 + c) * 32 + row + 8, :] = raw(3 + c) + timestep * halfway

    sums_refs = (sums0_ref, sums1_ref, sums2_ref, sums3_ref)
    for k in range(24):
        for sums_ref in sums_refs:
            sums_ref[k] = jnp.zeros((8, 128), jnp.float32)

    count = count_ref[0]
    keep = keep_ref[...]
    row = lax.broadcasted_iota(jnp.int32, (8, 128), 0)
    upper = row < 4
    first = (row & 3) * 32

    def spread(c, one, other):
        return jnp.where(
            upper,
            jnp.broadcast_to(ext_ref[pl.ds(c * 32 + one, 1), :], (8, 128)),
            jnp.broadcast_to(ext_ref[pl.ds(c * 32 + other, 1), :], (8, 128)),
        )

    def take_round(word, here, table, force):
        below = word - 1
        particle = (lax.population_count(below & ~word) + first) & 127
        there = [by_lane(table[c], particle) for c in range(6)]
        gap = [there[c] - here[c] for c in range(3)]
        now = [gap[c] + (there[3 + c] - here[3 + c]) for c in range(3)]
        rest2 = gap[0] * gap[0] + gap[1] * gap[1] + gap[2] * gap[2]
        now2 = now[0] * now[0] + now[1] * now[1] + now[2] * now[2]
        scaled = lax.rsqrt(rest2) - lax.rsqrt(now2)
        scaled = jnp.where(word != 0, scaled, 0.0)
        return word & below, [force[c] + scaled * now[c] for c in range(3)]

    def bonds(p):
        everything = jnp.where(pair_ref[0, p] == pair_ref[1, p], 0, -1)
        live = jnp.where(p < count, -1, 0)
        return bits_ref[pl.ds(p, 8, stride=pairs), :] & (keep | everything) & live

    def advance(u, p, word, rounds):
        home = (pair_ref[0, p], pair_ref[0, p + 1])
        away = (pair_ref[1, p], pair_ref[1, p + 1])
        here = [spread(c, *home) for c in range(6)]
        table = [spread(c, *away) for c in range(6)]
        force = [jnp.zeros((8, 128), jnp.float32) for _ in range(3)]
        for _ in range(rounds):
            word, force = take_round(word, here, table, force)
        left_ref[u] = word
        for c in range(3):
            sums_refs[u][home[0] * 3 + c] += jnp.where(upper, force[c], 0.0)
            sums_refs[u][home[1] * 3 + c] += jnp.where(upper, 0.0, force[c])

    def step(q, carry):
        for u in range(GROUP // 2):
            p = q * GROUP + 2 * u
            advance(u, p, jnp.where(upper, bonds(p), bonds(p + 1)), STEADY)

        def more(r, carry):
            for u in range(GROUP // 2):
                advance(u, q * GROUP + 2 * u, left_ref[u], 1)
            return carry

        lax.fori_loop(STEADY, rounds_ref[q], more, 0)
        return carry

    lax.fori_loop(0, (count + GROUP - 1) // GROUP, step, 0)

    for c in range(3):
        rows = [
            jnp.sum(sum(sums_ref[h * 3 + c] for sums_ref in sums_refs), axis=0, keepdims=True)
            for h in range(8)
        ]
        acceleration = stiffness * jnp.concatenate(rows, axis=0)
        acc_ref[c] = acceleration
        vel_ref[c] = vel_ref[c] + half_step * acceleration


def call_pack(owner, myself, fields):
    smem = pl.BlockSpec(memory_space=pltpu.SMEM)
    vmem = pl.BlockSpec(memory_space=pltpu.VMEM)
    return pl.pallas_call(
        pack_kernel,
        out_shape=jax.ShapeDtypeStruct((PACK, 128), jnp.float32),
        in_specs=[smem, smem] + [vmem] * 4,
        out_specs=vmem,
        name="pack",
    )(owner, myself, *fields)


def call_settle(picks, fields, candidates):
    smem = pl.BlockSpec(memory_space=pltpu.SMEM)
    vmem = pl.BlockSpec(memory_space=pltpu.VMEM)
    return pl.pallas_call(
        settle_kernel,
        out_shape=(
            jax.ShapeDtypeStruct((CELL, 128), jnp.float32),
            jax.ShapeDtypeStruct((8, 128), jnp.float32),
        ),
        in_specs=[smem] + [vmem] * 5,
        out_specs=(vmem, vmem),
        name="settle",
    )(picks, *fields, candidates)


def call_force(pair_blocks, pair_count, sources, around, far, bond_bits):
    smem = pl.BlockSpec(memory_space=pltpu.SMEM)
    vmem = pl.BlockSpec(memory_space=pltpu.VMEM)
    pairs = pair_blocks.shape[1]
    wide, rounds = call_prepare(bond_bits)
    keep = jnp.asarray(self_bits())
    tile = jax.ShapeDtypeStruct((3, 8, 128), jnp.float32)
    return pl.pallas_call(
        force_kernel,
        out_shape=(tile, tile, tile),
        in_specs=[smem] * 4 + [vmem] * 4,
        out_specs=(vmem, vmem, vmem),
        scratch_shapes=[
            pltpu.VMEM((COMPS * 24, 128), jnp.float32),
            pltpu.VMEM((6 * 32, 128), jnp.float32),
            pltpu.VMEM((GROUP // 2, 8, 128), jnp.int32),
        ]
        + [pltpu.VMEM((24, 8, 128), jnp.float32)] * 4,
        name="forces",
    )(
        pair_blocks,
        pair_count,
        sources,
        rounds,
        around,
        far,
        wide,
        keep,
    )


def shifted_by(shard, axis, amount):
    size = lax.axis_size(axis)
    return lax.ppermute(shard, axis, [(i, (i + amount) % size) for i in range(size)])


def highest(tiles):
    top = tiles[0]
    for tile in tiles[1:]:
        top = jnp.maximum(top, tile)
    return top


def around_index(offset, extent):
    wrapped = offset % extent
    return jnp.where(wrapped == 0, 1, jnp.where(wrapped == 1, 2, 0))


def choose(owner, myself, candidates, blocks):
    misc = candidates.reshape(27, PACK, 128)[:, 24, 0:4].astype(jnp.int32)
    own_ids = myself * blocks + jnp.arange(blocks, dtype=jnp.int32)
    owners = jnp.concatenate([owner, misc[:, 0:2].reshape(-1)])
    labels = jnp.concatenate([own_ids, misc[:, 2:4].reshape(-1)])
    chosen = owners == myself
    before = chosen[None, :] & (labels[None, :] < labels[:, None])
    ranked = jnp.sum(before.astype(jnp.int32), axis=1)
    places = jnp.arange(blocks, dtype=jnp.int32)
    matches = chosen[None, :] & (ranked[None, :] == places[:, None])
    numbers = jnp.arange(owners.shape[0], dtype=jnp.int32)
    return jnp.sum(jnp.where(matches, numbers[None, :], 0), axis=1)


def per_device(
    ref_pos,
    displace,
    velocity,
    acceleration,
    new_owner,
    ghost_ids,
    pair_blocks,
    pair_count,
    bond_bits,
):
    blocks = ref_pos.shape[0]
    size_x, size_y, size_z = (lax.axis_size(axis) for axis in AXES)
    place_x, place_y, place_z = (lax.axis_index(axis) for axis in AXES)
    myself = ((place_x * size_y + place_y) * size_z + place_z).astype(jnp.int32)
    fields = tuple(
        jnp.transpose(field, (1, 0, 2)) for field in (ref_pos, displace, velocity, acceleration)
    )

    body = call_pack(new_owner, myself[None], fields)
    for axis in AXES:
        before = shifted_by(body, axis, 1)
        after = shifted_by(body, axis, -1)
        body = jnp.concatenate([before, body, after], axis=0)
    picks = choose(new_owner, myself, body, blocks)
    around, top = call_settle(picks, fields, body)

    ghost_dev = ghost_ids // blocks
    ghost_slot = ghost_ids % blocks
    sources = (
        around_index(ghost_dev // (size_y * size_z) - place_x, size_x) * CELL
        + around_index(ghost_dev // size_z % size_y - place_y, size_y) * LINE
        + around_index(ghost_dev % size_z - place_z, size_z) * PLANE
        + ghost_slot
    ).astype(jnp.int32)
    x_axis, y_axis, z_axis = AXES
    before, after = shifted_by(around, x_axis, 1), shifted_by(around, x_axis, -1)
    far = shifted_by(top, x_axis, 4)
    top = highest([top, far, before[96:104], after[96:104]])
    around = jnp.concatenate([before, around, after, far], axis=0)

    before, after = shifted_by(around, y_axis, 1), shifted_by(around, y_axis, -1)
    far = shifted_by(top, y_axis, 4)
    tiles = [
        side[start : start + 8]
        for side in (before, after)
        for start in (96, CELL + 96, 2 * CELL + 96, 3 * CELL)
    ]
    top = highest([top, far] + tiles)
    around = jnp.concatenate([before, around, after, far], axis=0)

    before, after = shifted_by(around, z_axis, 1), shifted_by(around, z_axis, -1)
    far = shifted_by(top, z_axis, 4)
    around = jnp.concatenate([before, around, after], axis=0)
    outs = call_force(pair_blocks, pair_count, sources, around, far, bond_bits)
    return tuple(jnp.transpose(out, (1, 0, 2)) for out in outs)


def solution(mesh):
    wide = P(AXES, None, None)
    in_specs = (wide,) * 4 + (P(AXES), P(AXES), P(None, AXES), P(AXES), wide)
    return jax.shard_map(
        per_device, mesh=mesh, in_specs=in_specs, out_specs=(wide,) * 3, check_vma=False
    )
```

```python
import jax
import jax.numpy as jnp
import numpy as np
from jax import lax
from jax.experimental import pallas as pl
from jax.experimental.pallas import tpu as pltpu
from jax.sharding import Mesh
from jax.sharding import PartitionSpec as P

WORD_BITS = 11
GX = ("gx_half", "gx_odd")
GY = ("gy_half", "gy_odd")
GZ = ("gz_half", "gz_odd")
AXES = (GX, GY, GZ)
ALL = GX + GY + GZ
LATTICE = ("gx_half", "gy_half", "gz_half")

courant = 0.05
stiffness = 20.0


COMPS = 12
PACK = 32
CELL = 104
GROUP = 8
STEADY = 3


LANE_GATHER = lax.GatherDimensionNumbers(
    offset_dims=(),
    collapsed_slice_dims=(1,),
    start_index_map=(1,),
    operand_batching_dims=(0,),
    start_indices_batching_dims=(0,),
)


def by_lane(table, particle):
    return lax.gather(
        table,
        particle[:, :, None],
        LANE_GATHER,
        slice_sizes=(1, 1),
        mode=lax.GatherScatterMode.PROMISE_IN_BOUNDS,
    )


def prepare_kernel(words_ref, wide_ref, most_ref):
    pairs = words_ref.shape[1]

    def group(g, carry):
        start = pl.multiple_of(g * GROUP, GROUP)
        words = [words_ref[w, pl.ds(start, GROUP), :] for w in range(12)]
        most = None
        for t in range(4):
            total = None
            for w in range(12):
                move = WORD_BITS * w - 32 * t
                if -WORD_BITS < move < 32:
                    part = words[w] << move if move >= 0 else words[w] >> -move
                    total = part if total is None else total | part
            wide_ref[t, pl.ds(start, GROUP), :] = total
            wide_ref[4 + t, pl.ds(start, GROUP), :] = total
            used = lax.population_count(total)
            most = used if most is None else jnp.maximum(most, used)
        most_ref[pl.ds(g, 1), :] = jnp.full((1, 128), jnp.max(most), jnp.int32)
        return carry

    lax.fori_loop(0, pairs // GROUP, group, 0)


def call_prepare(bond_bits):
    pairs = bond_bits.shape[0]
    vmem = pl.BlockSpec(memory_space=pltpu.VMEM)
    wide, most = pl.pallas_call(
        prepare_kernel,
        out_shape=(
            jax.ShapeDtypeStruct((8, pairs, 128), jnp.int32),
            jax.ShapeDtypeStruct((pairs // GROUP, 128), jnp.int32),
        ),
        in_specs=[vmem],
        out_specs=(vmem, vmem),
        cost_estimate=pl.CostEstimate(
            flops=20_000_000, bytes_accessed=2_200_000, transcendentals=0
        ),
        name="prepare",
    )(jnp.transpose(bond_bits, (1, 0, 2)))
    return wide.reshape(8 * pairs, 128), most


def self_bits():
    bit = np.arange(128)[None, :] - 32 * (np.arange(8)[:, None] % 4)
    lost = np.where((bit >= 0) & (bit < 32), np.int64(1) << np.clip(bit, 0, 31), 0)
    return (~lost).astype(np.uint32).view(np.int32)


def pack_kernel(owner_ref, self_ref, ref_ref, dis_ref, vel_ref, acc_ref, out_ref, top_ref):
    myself = self_ref[0]
    first = jnp.int32(0)
    second = jnp.int32(0)
    found = jnp.bool_(False)
    for k in range(8):
        leaves = owner_ref[k] != myself
        first = jnp.where(leaves & jnp.logical_not(found), k, first)
        second = jnp.where(leaves & found, k, second)
        found = found | leaves
    for group, source in enumerate((ref_ref, dis_ref, vel_ref, acc_ref)):
        for c in range(3):
            out_ref[pl.ds(group * 3 + c, 1), :] = source[c, pl.ds(first, 1), :]
            out_ref[pl.ds(12 + group * 3 + c, 1), :] = source[c, pl.ds(second, 1), :]
    lane = lax.broadcasted_iota(jnp.int32, (8, 128), 1)
    values = (
        owner_ref[first],
        owner_ref[second],
        myself * 8 + first,
        myself * 8 + second,
    )
    misc = jnp.zeros((8, 128), jnp.float32)
    for place, value in enumerate(values):
        misc = jnp.where(lane == place, value.astype(jnp.float32), misc)
    speed = jnp.maximum(
        jnp.maximum(jnp.abs(vel_ref[0]), jnp.abs(vel_ref[1])), jnp.abs(vel_ref[2])
    )
    out_ref[24:32, :] = misc
    top_ref[...] = jnp.full(top_ref.shape, jnp.max(speed), jnp.float32)


def settle_kernel(
    owner_ref, self_ref, ref_ref, dis_ref, vel_ref, acc_ref, cand_ref, tops_ref, out_ref
):
    myself = self_ref[0]
    misc = cand_ref[pl.ds(24, 27, stride=PACK), :]
    lane = lax.broadcasted_iota(jnp.int32, misc.shape, 1)
    place = lax.broadcasted_iota(jnp.int32, misc.shape, 0) * 2 + lane
    labels = pltpu.roll(misc, 126, 1)
    mine = (lane < 2) & (misc == myself.astype(jnp.float32))
    none = 1e9
    keys = jnp.where(mine, labels * 64.0 + place.astype(jnp.float32), none)
    first_key = jnp.min(keys)
    first = first_key.astype(jnp.int32)
    second = jnp.min(jnp.where(keys > first_key, keys, none)).astype(jnp.int32)
    lower = (first >> 6 < myself * 8).astype(jnp.int32) + (second >> 6 < myself * 8).astype(
        jnp.int32
    )
    spots = (jnp.where(lower >= 1, 0, 6), jnp.where(lower == 2, 1, 7))
    sources = (ref_ref, dis_ref, vel_ref, acc_ref)
    slot = lower
    for k in range(8):
        stays = owner_ref[k] == myself
        target = jnp.where(stays, slot, spots[0])
        slot = slot + stays.astype(jnp.int32)
        for row in range(COMPS):
            out_ref[pl.ds(row * 8 + target, 1), :] = sources[row // 3][row % 3, k : k + 1, :]
    for key, spot in zip((first, second), spots):
        base = ((key & 63) >> 1) * PACK + (key & 1) * COMPS
        for row in range(COMPS):
            out_ref[pl.ds(row * 8 + spot, 1), :] = cand_ref[pl.ds(base + row, 1), :]
    out_ref[96:104, :] = jnp.broadcast_to(jnp.max(tops_ref[...], axis=0, keepdims=True), (8, 128))


def force_kernel(
    pair_ref,
    count_ref,
    source_ref,
    rounds_ref,
    around_ref,
    bits_ref,
    keep_ref,
    dis_ref,
    vel_ref,
    acc_ref,
    raw_ref,
    ext_ref,
    left_ref,
    sums0_ref,
    sums1_ref,
    sums2_ref,
    sums3_ref,
):
    pairs = pair_ref.shape[1]
    fastest = around_ref[96:104, :]
    for cell in range(1, 27):
        fastest = jnp.maximum(fastest, around_ref[cell * CELL + 96 : cell * CELL + 104, :])
    timestep = courant / (fastest + 1e-06)
    half_step = 0.5 * timestep

    def own(c):
        start = 13 * CELL + 8 * c
        return around_ref[start : start + 8, :]

    for c in range(3):
        halfway = own(6 + c) + half_step * own(9 + c)
        shifted = own(3 + c) + timestep * halfway
        dis_ref[c] = shifted
        vel_ref[c] = halfway
        ext_ref[c * 32 : c * 32 + 8, :] = own(c)
        ext_ref[(3 + c) * 32 : (3 + c) * 32 + 8, :] = shifted

    for g in range(24):
        start = source_ref[g]
        for c in range(COMPS):
            raw_ref[c * 24 + g : c * 24 + g + 1, :] = around_ref[pl.ds(start + 8 * c, 1), :]

    for c in range(3):
        for t in range(3):

            def raw(n):
                return raw_ref[n * 24 + t * 8 : n * 24 + t * 8 + 8, :]

            halfway = raw(6 + c) + half_step * raw(9 + c)
            row = 8 + t * 8
            ext_ref[c * 32 + row : c * 32 + row + 8, :] = raw(c)
            ext_ref[(3 + c) * 32 + row : (3 + c) * 32 + row + 8, :] = raw(3 + c) + timestep * halfway

    sums_refs = (sums0_ref, sums1_ref, sums2_ref, sums3_ref)
    for k in range(24):
        for sums_ref in sums_refs:
            sums_ref[k] = jnp.zeros((8, 128), jnp.float32)

    count = count_ref[0]
    keep = keep_ref[...]
    row = lax.broadcasted_iota(jnp.int32, (8, 128), 0)
    upper = row < 4
    first = (row & 3) * 32

    def spread(c, one, other):
        return jnp.where(
            upper,
            jnp.broadcast_to(ext_ref[pl.ds(c * 32 + one, 1), :], (8, 128)),
            jnp.broadcast_to(ext_ref[pl.ds(c * 32 + other, 1), :], (8, 128)),
        )

    def take_round(word, here, table, force):
        below = word - 1
        particle = (lax.population_count(below & ~word) + first) & 127
        there = [by_lane(table[c], particle) for c in range(6)]
        gap = [there[c] - here[c] for c in range(3)]
        now = [gap[c] + (there[3 + c] - here[3 + c]) for c in range(3)]
        rest2 = gap[0] * gap[0] + gap[1] * gap[1] + gap[2] * gap[2]
        now2 = now[0] * now[0] + now[1] * now[1] + now[2] * now[2]
        scaled = lax.rsqrt(rest2) - lax.rsqrt(now2)
        scaled = jnp.where(word != 0, scaled, 0.0)
        return word & below, [force[c] + scaled * now[c] for c in range(3)]

    def bonds(p):
        everything = jnp.where(pair_ref[0, p] == pair_ref[1, p], 0, -1)
        live = jnp.where(p < count, -1, 0)
        return bits_ref[pl.ds(p, 8, stride=pairs), :] & (keep | everything) & live

    def advance(u, p, word, rounds):
        home = (pair_ref[0, p], pair_ref[0, p + 1])
        away = (pair_ref[1, p], pair_ref[1, p + 1])
        here = [spread(c, *home) for c in range(6)]
        table = [spread(c, *away) for c in range(6)]
        force = [jnp.zeros((8, 128), jnp.float32) for _ in range(3)]
        for _ in range(rounds):
            word, force = take_round(word, here, table, force)
        left_ref[u] = word
        for c in range(3):
            sums_refs[u][home[0] * 3 + c] += jnp.where(upper, force[c], 0.0)
            sums_refs[u][home[1] * 3 + c] += jnp.where(upper, 0.0, force[c])

    def step(q, carry):
        for u in range(GROUP // 2):
            p = q * GROUP + 2 * u
            advance(u, p, jnp.where(upper, bonds(p), bonds(p + 1)), STEADY)

        def more(r, carry):
            for u in range(GROUP // 2):
                advance(u, q * GROUP + 2 * u, left_ref[u], 1)
            return carry

        lax.fori_loop(STEADY, rounds_ref[q, 0], more, 0)
        return carry

    lax.fori_loop(0, (count + GROUP - 1) // GROUP, step, 0)

    for c in range(3):
        rows = [
            jnp.sum(sum(sums_ref[h * 3 + c] for sums_ref in sums_refs), axis=0, keepdims=True)
            for h in range(8)
        ]
        acceleration = stiffness * jnp.concatenate(rows, axis=0)
        acc_ref[c] = acceleration
        vel_ref[c] = vel_ref[c] + half_step * acceleration


def call_pack(owner, myself, fields, lattice):
    smem = pl.BlockSpec(memory_space=pltpu.SMEM)
    vmem = pl.BlockSpec(memory_space=pltpu.VMEM)
    return pl.pallas_call(
        pack_kernel,
        out_shape=(
            jax.ShapeDtypeStruct((PACK, 128), jnp.float32),
            jax.ShapeDtypeStruct((lattice, 128), jnp.float32),
        ),
        in_specs=[smem, smem] + [vmem] * 4,
        out_specs=(vmem, vmem),
        name="pack",
    )(owner, myself, *fields)


def call_settle(owner, myself, fields, candidates, tops):
    smem = pl.BlockSpec(memory_space=pltpu.SMEM)
    vmem = pl.BlockSpec(memory_space=pltpu.VMEM)
    return pl.pallas_call(
        settle_kernel,
        out_shape=jax.ShapeDtypeStruct((CELL, 128), jnp.float32),
        in_specs=[smem, smem] + [vmem] * 6,
        out_specs=vmem,
        name="settle",
    )(owner, myself, *fields, candidates, tops)


def call_force(pair_blocks, pair_count, sources, around, wide, rounds):
    smem = pl.BlockSpec(memory_space=pltpu.SMEM)
    vmem = pl.BlockSpec(memory_space=pltpu.VMEM)
    keep = jnp.asarray(self_bits())
    tile = jax.ShapeDtypeStruct((3, 8, 128), jnp.float32)
    return pl.pallas_call(
        force_kernel,
        out_shape=(tile, tile, tile),
        in_specs=[smem] * 4 + [vmem] * 3,
        out_specs=(vmem, vmem, vmem),
        scratch_shapes=[
            pltpu.VMEM((COMPS * 24, 128), jnp.float32),
            pltpu.VMEM((6 * 32, 128), jnp.float32),
            pltpu.VMEM((GROUP // 2, 8, 128), jnp.int32),
        ]
        + [pltpu.VMEM((24, 8, 128), jnp.float32)] * 4,
        name="forces",
    )(
        pair_blocks,
        pair_count,
        sources,
        rounds,
        around,
        wide,
        keep,
    )


def shifted_by(shard, axis, amount):
    size = lax.axis_size(axis)
    return lax.ppermute(shard, axis, [(i, (i + amount) % size) for i in range(size)])


def around_index(offset, extent):
    wrapped = offset % extent
    return jnp.where(wrapped == 0, 1, jnp.where(wrapped == 1, 2, 0))


def per_device(
    ref_pos,
    displace,
    velocity,
    acceleration,
    new_owner,
    ghost_ids,
    pair_blocks,
    pair_count,
    bond_bits,
):
    blocks = ref_pos.shape[0]
    size_x, size_y, size_z = (lax.axis_size(axis) for axis in AXES)
    place_x, place_y, place_z = (lax.axis_index(axis) for axis in AXES)
    myself = ((place_x * size_y + place_y) * size_z + place_z).astype(jnp.int32)
    fields = tuple(
        jnp.transpose(field, (1, 0, 2)) for field in (ref_pos, displace, velocity, acceleration)
    )

    lattice = lax.axis_size(LATTICE)
    body, tops = call_pack(new_owner, myself[None], fields, lattice)
    tops = lax.all_to_all(tops, LATTICE, 0, 0, tiled=True)
    for axis in AXES:
        before = shifted_by(body, axis, 1)
        after = shifted_by(body, axis, -1)
        body = jnp.concatenate([before, body, after], axis=0)
    around = call_settle(new_owner, myself[None], fields, body, tops)

    ghost_dev = ghost_ids // blocks
    ghost_slot = ghost_ids % blocks
    sources = (
        around_index(ghost_dev // (size_y * size_z) - place_x, size_x)
        + around_index(ghost_dev // size_z % size_y - place_y, size_y) * 3
        + around_index(ghost_dev % size_z - place_z, size_z) * 9
    ) * CELL + ghost_slot
    sources = sources.astype(jnp.int32)
    for axis in AXES:
        before = shifted_by(around, axis, 1)
        after = shifted_by(around, axis, -1)
        around = jnp.concatenate([before, around, after], axis=0)
    wide, rounds = call_prepare(bond_bits)
    outs = call_force(pair_blocks, pair_count, sources, around, wide, rounds)
    return tuple(jnp.transpose(out, (1, 0, 2)) for out in outs)


def solution(mesh):
    sizes = [mesh.shape[axis] for axis in ("gx", "gy", "gz")]
    split = Mesh(mesh.devices.reshape([n for size in sizes for n in (size // 2, 2)]), ALL)
    wide = P(ALL, None, None)
    in_specs = (wide,) * 4 + (P(ALL), P(ALL), P(None, ALL), P(ALL), wide)

    return jax.shard_map(
        per_device, mesh=split, in_specs=in_specs, out_specs=(wide,) * 3, check_vma=False
    )
```

```python
import jax
import jax.numpy as jnp
import numpy as np
from jax import lax
from jax.experimental import pallas as pl
from jax.experimental.pallas import tpu as pltpu
from jax.sharding import Mesh
from jax.sharding import PartitionSpec as P

WORD_BITS = 11
GX = ("gx_half", "gx_rest")
GY = ("gy_half", "gy_rest")
GZ = ("gz_half", "gz_rest")
AXES = (GX, GY, GZ)
ALL = GX + GY + GZ
HALVES = ("gx_half", "gy_half", "gz_half")

courant = 0.05
stiffness = 20.0


COMPS = 12
PACK = 32
CELL = 104
GROUP = 8
STEADY = 3


LANE_GATHER = lax.GatherDimensionNumbers(
    offset_dims=(),
    collapsed_slice_dims=(1,),
    start_index_map=(1,),
    operand_batching_dims=(0,),
    start_indices_batching_dims=(0,),
)


def by_lane(table, particle):
    return lax.gather(
        table,
        particle[:, :, None],
        LANE_GATHER,
        slice_sizes=(1, 1),
        mode=lax.GatherScatterMode.PROMISE_IN_BOUNDS,
    )


def prepare_kernel(words_ref, wide_ref, most_ref):
    pairs = words_ref.shape[1]

    def group(g, carry):
        start = pl.multiple_of(g * GROUP, GROUP)
        words = [words_ref[w, pl.ds(start, GROUP), :] for w in range(12)]
        most = None
        for t in range(4):
            total = None
            for w in range(12):
                move = WORD_BITS * w - 32 * t
                if -WORD_BITS < move < 32:
                    part = words[w] << move if move >= 0 else words[w] >> -move
                    total = part if total is None else total | part
            wide_ref[t, pl.ds(start, GROUP), :] = total
            wide_ref[4 + t, pl.ds(start, GROUP), :] = total
            used = lax.population_count(total)
            most = used if most is None else jnp.maximum(most, used)
        most_ref[pl.ds(g, 1), :] = jnp.max(most, axis=0, keepdims=True)
        return carry

    lax.fori_loop(0, pairs // GROUP, group, 0, unroll=3)
    most_ref[...] = jnp.broadcast_to(
        jnp.max(most_ref[...], axis=1, keepdims=True), most_ref.shape
    )


def call_prepare(bond_bits):
    pairs = bond_bits.shape[0]
    wide, most = pl.pallas_call(
        prepare_kernel,
        out_shape=(
            pltpu.VMEM((8, pairs, 128), jnp.int32),
            jax.ShapeDtypeStruct((pairs // GROUP, 128), jnp.int32),
        ),
        in_specs=[VMEM],
        out_specs=(VMEM, VMEM),
        cost_estimate=pl.CostEstimate(
            flops=20_000_000, bytes_accessed=2_200_000, transcendentals=0
        ),
        compiler_params=LITTLE,
        name="prepare",
    )(jnp.transpose(bond_bits, (1, 0, 2)))
    return wide.reshape(8 * pairs, 128), most


def self_bits():
    bit = np.arange(128)[None, :] - 32 * (np.arange(8)[:, None] % 4)
    lost = np.where((bit >= 0) & (bit < 32), np.int64(1) << np.clip(bit, 0, 31), 0)
    return (~lost).astype(np.uint32).view(np.int32)


def pack_kernel(
    owner_ref, self_ref, tops_ref, ref_ref, dis_ref, vel_ref, acc_ref, out_ref
):
    myself = self_ref[0]
    first = jnp.int32(0)
    second = jnp.int32(0)
    found = jnp.bool_(False)
    for k in range(8):
        leaves = owner_ref[k] != myself
        first = jnp.where(leaves & jnp.logical_not(found), k, first)
        second = jnp.where(leaves & found, k, second)
        found = found | leaves
    for group, source in enumerate((ref_ref, dis_ref, vel_ref, acc_ref)):
        for c in range(3):
            out_ref[pl.ds(group * 3 + c, 1), :] = source[c, pl.ds(first, 1), :]
            out_ref[pl.ds(12 + group * 3 + c, 1), :] = source[c, pl.ds(second, 1), :]
    lane = lax.broadcasted_iota(jnp.int32, (8, 128), 1)
    values = (
        owner_ref[first],
        owner_ref[second],
        myself * 8 + first,
        myself * 8 + second,
    )
    misc = jnp.zeros((8, 128), jnp.float32)
    for place, value in enumerate(values):
        misc = jnp.where(lane == place, value.astype(jnp.float32), misc)
    row = lax.broadcasted_iota(jnp.int32, (8, 128), 0)
    top = jnp.max(tops_ref[...], axis=0, keepdims=True)
    out_ref[24:32, :] = jnp.where(row == 0, misc, top)


def settle_kernel(
    owner_ref, self_ref, ref_ref, dis_ref, vel_ref, acc_ref, cand_ref, out_ref
):
    myself = self_ref[0]
    misc = cand_ref[pl.ds(24, 27, stride=PACK), :]
    lane = lax.broadcasted_iota(jnp.int32, misc.shape, 1)
    place = lax.broadcasted_iota(jnp.int32, misc.shape, 0) * 2 + lane
    labels = pltpu.roll(misc, 126, 1)
    mine = (lane < 2) & (misc == myself.astype(jnp.float32))
    none = 1e9
    keys = jnp.where(mine, labels * 64.0 + place.astype(jnp.float32), none)
    first_key = jnp.min(keys)
    first = first_key.astype(jnp.int32)
    second = jnp.min(jnp.where(keys > first_key, keys, none)).astype(jnp.int32)
    lower = (first >> 6 < myself * 8).astype(jnp.int32) + (second >> 6 < myself * 8).astype(
        jnp.int32
    )
    spots = (jnp.where(lower >= 1, 0, 6), jnp.where(lower == 2, 1, 7))
    sources = (ref_ref, dis_ref, vel_ref, acc_ref)
    slot = lower
    for k in range(8):
        stays = owner_ref[k] == myself
        target = jnp.where(stays, slot, spots[0])
        slot = slot + stays.astype(jnp.int32)
        for row in range(COMPS):
            out_ref[pl.ds(row * 8 + target, 1), :] = sources[row // 3][row % 3, k : k + 1, :]
    for key, spot in zip((first, second), spots):
        base = ((key & 63) >> 1) * PACK + (key & 1) * COMPS
        for row in range(COMPS):
            out_ref[pl.ds(row * 8 + spot, 1), :] = cand_ref[pl.ds(base + row, 1), :]
    tops = cand_ref[pl.ds(25, 27, stride=PACK), :]
    out_ref[96:104, :] = jnp.broadcast_to(jnp.max(tops, axis=0, keepdims=True), (8, 128))


def force_kernel(
    pair_ref,
    count_ref,
    source_ref,
    rounds_ref,
    around_ref,
    bits_ref,
    keep_ref,
    dis_ref,
    vel_ref,
    acc_ref,
    raw_ref,
    ext_ref,
    left_ref,
    sums0_ref,
    sums1_ref,
    sums2_ref,
    sums3_ref,
):
    pairs = pair_ref.shape[1]
    fastest = around_ref[96:104, :]
    for cell in range(1, 27):
        fastest = jnp.maximum(fastest, around_ref[cell * CELL + 96 : cell * CELL + 104, :])
    timestep = courant / (fastest + 1e-06)
    half_step = 0.5 * timestep

    def own(c):
        start = 13 * CELL + 8 * c
        return around_ref[start : start + 8, :]

    for c in range(3):
        halfway = own(6 + c) + half_step * own(9 + c)
        shifted = own(3 + c) + timestep * halfway
        dis_ref[c] = shifted
        vel_ref[c] = halfway
        ext_ref[c * 32 : c * 32 + 8, :] = own(c)
        ext_ref[(3 + c) * 32 : (3 + c) * 32 + 8, :] = shifted

    for g in range(24):
        start = source_ref[g]
        for c in range(COMPS):
            raw_ref[c * 24 + g : c * 24 + g + 1, :] = around_ref[pl.ds(start + 8 * c, 1), :]

    for c in range(3):
        for t in range(3):

            def raw(n):
                return raw_ref[n * 24 + t * 8 : n * 24 + t * 8 + 8, :]

            halfway = raw(6 + c) + half_step * raw(9 + c)
            row = 8 + t * 8
            ext_ref[c * 32 + row : c * 32 + row + 8, :] = raw(c)
            ext_ref[(3 + c) * 32 + row : (3 + c) * 32 + row + 8, :] = raw(3 + c) + timestep * halfway

    sums_refs = (sums0_ref, sums1_ref, sums2_ref, sums3_ref)
    for k in range(24):
        for sums_ref in sums_refs:
            sums_ref[k] = jnp.zeros((8, 128), jnp.float32)

    count = count_ref[0]
    keep = keep_ref[...]
    row = lax.broadcasted_iota(jnp.int32, (8, 128), 0)
    upper = row < 4
    first = (row & 3) * 32

    def spread(c, one, other):
        return jnp.where(
            upper,
            jnp.broadcast_to(ext_ref[pl.ds(c * 32 + one, 1), :], (8, 128)),
            jnp.broadcast_to(ext_ref[pl.ds(c * 32 + other, 1), :], (8, 128)),
        )

    def take_round(word, here, table, force):
        below = word - 1
        particle = (lax.population_count(below & ~word) + first) & 127
        there = [by_lane(table[c], particle) for c in range(6)]
        gap = [there[c] - here[c] for c in range(3)]
        now = [gap[c] + (there[3 + c] - here[3 + c]) for c in range(3)]
        rest2 = gap[0] * gap[0] + gap[1] * gap[1] + gap[2] * gap[2]
        now2 = now[0] * now[0] + now[1] * now[1] + now[2] * now[2]
        scaled = lax.rsqrt(rest2) - lax.rsqrt(now2)
        scaled = jnp.where(word != 0, scaled, 0.0)
        return word & below, [force[c] + scaled * now[c] for c in range(3)]

    def bonds(p):
        everything = jnp.where(pair_ref[0, p] == pair_ref[1, p], 0, -1)
        live = jnp.where(p < count, -1, 0)
        return bits_ref[pl.ds(p, 8, stride=pairs), :] & (keep | everything) & live

    def advance(u, p, word, rounds):
        home = (pair_ref[0, p], pair_ref[0, p + 1])
        away = (pair_ref[1, p], pair_ref[1, p + 1])
        here = [spread(c, *home) for c in range(6)]
        table = [spread(c, *away) for c in range(6)]
        force = [jnp.zeros((8, 128), jnp.float32) for _ in range(3)]
        for _ in range(rounds):
            word, force = take_round(word, here, table, force)
        left_ref[u] = word
        for c in range(3):
            sums_refs[u][home[0] * 3 + c] += jnp.where(upper, force[c], 0.0)
            sums_refs[u][home[1] * 3 + c] += jnp.where(upper, 0.0, force[c])

    def step(q, carry):
        for u in range(GROUP // 2):
            p = q * GROUP + 2 * u
            advance(u, p, jnp.where(upper, bonds(p), bonds(p + 1)), STEADY)

        def more(r, carry):
            for u in range(GROUP // 2):
                advance(u, q * GROUP + 2 * u, left_ref[u], 1)
            return carry

        lax.fori_loop(STEADY, rounds_ref[q, 0], more, 0)
        return carry

    lax.fori_loop(0, (count + GROUP - 1) // GROUP, step, 0)

    for c in range(3):
        rows = [
            jnp.sum(sum(sums_ref[h * 3 + c] for sums_ref in sums_refs), axis=0, keepdims=True)
            for h in range(8)
        ]
        acceleration = stiffness * jnp.concatenate(rows, axis=0)
        acc_ref[c] = acceleration
        vel_ref[c] = vel_ref[c] + half_step * acceleration


SMEM = pl.BlockSpec(memory_space=pltpu.SMEM)
VMEM = pl.BlockSpec(memory_space=pltpu.VMEM)


LITTLE = pltpu.CompilerParams(vmem_limit_bytes=8 * 1024 * 1024)


def near(value):
    return pltpu.with_memory_space_constraint(value, pltpu.VMEM)


def call_pack(owner, myself, tops, fields):
    return pl.pallas_call(
        pack_kernel,
        out_shape=pltpu.VMEM((PACK, 128), jnp.float32),
        in_specs=[SMEM, SMEM] + [VMEM] * 5,
        out_specs=VMEM,
        compiler_params=LITTLE,
        name="pack",
    )(owner, myself, near(tops), *fields)


def call_settle(owner, myself, fields, candidates):
    return pl.pallas_call(
        settle_kernel,
        out_shape=pltpu.VMEM((CELL, 128), jnp.float32),
        in_specs=[SMEM, SMEM] + [VMEM] * 5,
        out_specs=VMEM,
        compiler_params=LITTLE,
        name="settle",
    )(owner, myself, *fields, near(candidates))


def call_force(pair_blocks, pair_count, sources, around, wide, rounds):
    keep = jnp.asarray(self_bits())
    tile = jax.ShapeDtypeStruct((3, 8, 128), jnp.float32)
    return pl.pallas_call(
        force_kernel,
        out_shape=(tile, tile, tile),
        in_specs=[SMEM] * 4 + [VMEM] * 3,
        out_specs=(VMEM, VMEM, VMEM),
        scratch_shapes=[
            pltpu.VMEM((COMPS * 24, 128), jnp.float32),
            pltpu.VMEM((6 * 32, 128), jnp.float32),
            pltpu.VMEM((GROUP // 2, 8, 128), jnp.int32),
        ]
        + [pltpu.VMEM((24, 8, 128), jnp.float32)] * 4,
        compiler_params=LITTLE,
        name="forces",
    )(
        pair_blocks,
        pair_count,
        sources,
        rounds,
        near(around),
        near(wide),
        keep,
    )


def shifted_by(shard, axis, amount):
    size = lax.axis_size(axis)
    return lax.ppermute(shard, axis, [(i, (i + amount) % size) for i in range(size)])


def around_index(offset, extent):
    wrapped = offset % extent
    return jnp.where(wrapped == 0, 1, jnp.where(wrapped == 1, 2, 0))


def per_device(
    ref_pos,
    displace,
    velocity,
    acceleration,
    new_owner,
    ghost_ids,
    pair_blocks,
    pair_count,
    bond_bits,
):
    blocks = ref_pos.shape[0]
    size_x, size_y, size_z = (lax.axis_size(axis) for axis in AXES)
    place_x, place_y, place_z = (lax.axis_index(axis) for axis in AXES)
    myself = ((place_x * size_y + place_y) * size_z + place_z).astype(jnp.int32)
    fields = tuple(
        jnp.transpose(field, (1, 0, 2)) for field in (ref_pos, displace, velocity, acceleration)
    )

    fastest = jnp.max(jnp.abs(velocity))
    tops = lax.all_to_all(jnp.broadcast_to(fastest, (8, 128)), HALVES, 0, 0, tiled=True)
    body = call_pack(new_owner, myself[None], tops, fields)
    for axis in AXES:
        before = shifted_by(body, axis, 1)
        after = shifted_by(body, axis, -1)
        body = jnp.concatenate([before, body, after], axis=0)
    around = call_settle(new_owner, myself[None], fields, body)

    ghost_dev = ghost_ids // blocks
    ghost_slot = ghost_ids % blocks
    sources = (
        around_index(ghost_dev // (size_y * size_z) - place_x, size_x)
        + around_index(ghost_dev // size_z % size_y - place_y, size_y) * 3
        + around_index(ghost_dev % size_z - place_z, size_z) * 9
    ) * CELL + ghost_slot
    sources = sources.astype(jnp.int32)
    for axis in AXES:
        before = shifted_by(around, axis, 1)
        after = shifted_by(around, axis, -1)
        around = jnp.concatenate([before, around, after], axis=0)
    wide, rounds = call_prepare(bond_bits)
    outs = call_force(pair_blocks, pair_count, sources, around, wide, rounds)
    return tuple(jnp.transpose(out, (1, 0, 2)) for out in outs)


def solution(mesh):
    sizes = [mesh.shape[axis] for axis in ("gx", "gy", "gz")]
    split = Mesh(mesh.devices.reshape([n for size in sizes for n in (2, size // 2)]), ALL)
    wide = P(ALL, None, None)
    in_specs = (wide,) * 4 + (P(ALL), P(ALL), P(None, ALL), P(ALL), wide)

    return jax.shard_map(
        per_device, mesh=split, in_specs=in_specs, out_specs=(wide,) * 3, check_vma=False
    )
```

```python
import jax
import jax.numpy as jnp
import numpy as np
from jax import lax
from jax.experimental import pallas as pl
from jax.experimental.pallas import tpu as pltpu
from jax.sharding import Mesh
from jax.sharding import PartitionSpec as P

WORD_BITS = 11
GX = ("gx_half", "gx_odd")
GY = ("gy_half", "gy_odd")
GZ = ("gz_half", "gz_odd")
AXES = (GX, GY, GZ)
ALL = GX + GY + GZ
LATTICE = ("gx_half", "gy_half", "gz_half")

courant = 0.05
stiffness = 20.0


COMPS = 12
PACK = 32
CELL = 96
GROUP = 8
STEADY = 3


LANE_GATHER = lax.GatherDimensionNumbers(
    offset_dims=(),
    collapsed_slice_dims=(1,),
    start_index_map=(1,),
    operand_batching_dims=(0,),
    start_indices_batching_dims=(0,),
)


def by_lane(table, particle):
    return lax.gather(
        table,
        particle[:, :, None],
        LANE_GATHER,
        slice_sizes=(1, 1),
        mode=lax.GatherScatterMode.PROMISE_IN_BOUNDS,
    )


def prepare_kernel(words_ref, wide_ref, most_ref):
    pairs = words_ref.shape[1]

    def group(g, carry):
        start = pl.multiple_of(g * GROUP, GROUP)
        words = [words_ref[w, pl.ds(start, GROUP), :] for w in range(12)]
        most = None
        for t in range(4):
            total = None
            for w in range(12):
                move = WORD_BITS * w - 32 * t
                if -WORD_BITS < move < 32:
                    part = words[w] << move if move >= 0 else words[w] >> -move
                    total = part if total is None else total | part
            wide_ref[t, pl.ds(start, GROUP), :] = total
            wide_ref[4 + t, pl.ds(start, GROUP), :] = total
            used = lax.population_count(total)
            most = used if most is None else jnp.maximum(most, used)
        most_ref[pl.ds(g, 1), :] = jnp.max(most, axis=0, keepdims=True)
        return carry

    lax.fori_loop(0, pairs // GROUP, group, 0, unroll=3)
    most_ref[...] = jnp.broadcast_to(
        jnp.max(most_ref[...], axis=1, keepdims=True), most_ref.shape
    )


def call_prepare(bond_bits):
    pairs = bond_bits.shape[0]
    wide, most = pl.pallas_call(
        prepare_kernel,
        out_shape=(
            pltpu.VMEM((8, pairs, 128), jnp.int32),
            jax.ShapeDtypeStruct((pairs // GROUP, 128), jnp.int32),
        ),
        in_specs=[VMEM],
        out_specs=(VMEM, VMEM),
        cost_estimate=pl.CostEstimate(
            flops=20_000_000, bytes_accessed=2_200_000, transcendentals=0
        ),
        compiler_params=LITTLE,
        name="prepare",
    )(jnp.transpose(bond_bits, (1, 0, 2)))
    return wide.reshape(8 * pairs, 128), most


def self_bits():
    bit = np.arange(128)[None, :] - 32 * (np.arange(8)[:, None] % 4)
    lost = np.where((bit >= 0) & (bit < 32), np.int64(1) << np.clip(bit, 0, 31), 0)
    return (~lost).astype(np.uint32).view(np.int32)


def pack_kernel(owner_ref, self_ref, ref_ref, dis_ref, vel_ref, acc_ref, out_ref):
    myself = self_ref[0]
    first = jnp.int32(0)
    second = jnp.int32(0)
    found = jnp.bool_(False)
    for k in range(8):
        leaves = owner_ref[k] != myself
        first = jnp.where(leaves & jnp.logical_not(found), k, first)
        second = jnp.where(leaves & found, k, second)
        found = found | leaves
    for group, source in enumerate((ref_ref, dis_ref, vel_ref, acc_ref)):
        for c in range(3):
            out_ref[pl.ds(group * 3 + c, 1), :] = source[c, pl.ds(first, 1), :]
            out_ref[pl.ds(12 + group * 3 + c, 1), :] = source[c, pl.ds(second, 1), :]
    lane = lax.broadcasted_iota(jnp.int32, (8, 128), 1)
    values = (
        owner_ref[first],
        owner_ref[second],
        myself * 8 + first,
        myself * 8 + second,
    )
    misc = jnp.zeros((8, 128), jnp.float32)
    for place, value in enumerate(values):
        misc = jnp.where(lane == place, value.astype(jnp.float32), misc)
    row = lax.broadcasted_iota(jnp.int32, (8, 128), 0)
    speed = jnp.maximum(
        jnp.maximum(jnp.abs(vel_ref[0]), jnp.abs(vel_ref[1])), jnp.abs(vel_ref[2])
    )
    out_ref[24:32, :] = jnp.where(row == 0, misc, jnp.max(speed))


def settle_kernel(
    owner_ref, self_ref, ref_ref, dis_ref, vel_ref, acc_ref, cand_ref, out_ref, top_ref
):
    myself = self_ref[0]
    misc = cand_ref[pl.ds(24, 27, stride=PACK), :]
    lane = lax.broadcasted_iota(jnp.int32, misc.shape, 1)
    place = lax.broadcasted_iota(jnp.int32, misc.shape, 0) * 2 + lane
    labels = pltpu.roll(misc, 126, 1)
    mine = (lane < 2) & (misc == myself.astype(jnp.float32))
    none = 1e9
    keys = jnp.where(mine, labels * 64.0 + place.astype(jnp.float32), none)
    first_key = jnp.min(keys)
    first = first_key.astype(jnp.int32)
    second = jnp.min(jnp.where(keys > first_key, keys, none)).astype(jnp.int32)
    lower = (first >> 6 < myself * 8).astype(jnp.int32) + (second >> 6 < myself * 8).astype(
        jnp.int32
    )
    spots = (jnp.where(lower >= 1, 0, 6), jnp.where(lower == 2, 1, 7))
    sources = (ref_ref, dis_ref, vel_ref, acc_ref)
    slot = lower
    for k in range(8):
        stays = owner_ref[k] == myself
        target = jnp.where(stays, slot, spots[0])
        slot = slot + stays.astype(jnp.int32)
        for row in range(COMPS):
            out_ref[pl.ds(row * 8 + target, 1), :] = sources[row // 3][row % 3, k : k + 1, :]
    for key, spot in zip((first, second), spots):
        base = ((key & 63) >> 1) * PACK + (key & 1) * COMPS
        for row in range(COMPS):
            out_ref[pl.ds(row * 8 + spot, 1), :] = cand_ref[pl.ds(base + row, 1), :]
    tops = cand_ref[pl.ds(25, 27, stride=PACK), :]
    top_ref[...] = jnp.broadcast_to(jnp.max(tops, axis=0, keepdims=True), top_ref.shape)


def force_kernel(
    pair_ref,
    count_ref,
    source_ref,
    rounds_ref,
    around_ref,
    tops_ref,
    bits_ref,
    keep_ref,
    dis_ref,
    vel_ref,
    acc_ref,
    raw_ref,
    ext_ref,
    left_ref,
    sums0_ref,
    sums1_ref,
    sums2_ref,
    sums3_ref,
):
    pairs = pair_ref.shape[1]
    fastest = jnp.broadcast_to(jnp.max(tops_ref[...], axis=0, keepdims=True), (8, 128))
    timestep = courant / (fastest + 1e-06)
    half_step = 0.5 * timestep

    def own(c):
        start = 13 * CELL + 8 * c
        return around_ref[start : start + 8, :]

    for c in range(3):
        halfway = own(6 + c) + half_step * own(9 + c)
        shifted = own(3 + c) + timestep * halfway
        dis_ref[c] = shifted
        vel_ref[c] = halfway
        ext_ref[c * 32 : c * 32 + 8, :] = own(c)
        ext_ref[(3 + c) * 32 : (3 + c) * 32 + 8, :] = shifted

    for g in range(24):
        start = source_ref[g]
        for c in range(COMPS):
            raw_ref[c * 24 + g : c * 24 + g + 1, :] = around_ref[pl.ds(start + 8 * c, 1), :]

    for c in range(3):
        for t in range(3):

            def raw(n):
                return raw_ref[n * 24 + t * 8 : n * 24 + t * 8 + 8, :]

            halfway = raw(6 + c) + half_step * raw(9 + c)
            row = 8 + t * 8
            ext_ref[c * 32 + row : c * 32 + row + 8, :] = raw(c)
            ext_ref[(3 + c) * 32 + row : (3 + c) * 32 + row + 8, :] = raw(3 + c) + timestep * halfway

    sums_refs = (sums0_ref, sums1_ref, sums2_ref, sums3_ref)
    for k in range(24):
        for sums_ref in sums_refs:
            sums_ref[k] = jnp.zeros((8, 128), jnp.float32)

    count = count_ref[0]
    keep = keep_ref[...]
    row = lax.broadcasted_iota(jnp.int32, (8, 128), 0)
    upper = row < 4
    first = (row & 3) * 32

    def spread(c, one, other):
        return jnp.where(
            upper,
            jnp.broadcast_to(ext_ref[pl.ds(c * 32 + one, 1), :], (8, 128)),
            jnp.broadcast_to(ext_ref[pl.ds(c * 32 + other, 1), :], (8, 128)),
        )

    def take_round(word, here, table, force):
        below = word - 1
        particle = (lax.population_count(below & ~word) + first) & 127
        there = [by_lane(table[c], particle) for c in range(6)]
        gap = [there[c] - here[c] for c in range(3)]
        now = [gap[c] + (there[3 + c] - here[3 + c]) for c in range(3)]
        rest2 = gap[0] * gap[0] + gap[1] * gap[1] + gap[2] * gap[2]
        now2 = now[0] * now[0] + now[1] * now[1] + now[2] * now[2]
        scaled = lax.rsqrt(rest2) - lax.rsqrt(now2)
        scaled = jnp.where(word != 0, scaled, 0.0)
        return word & below, [force[c] + scaled * now[c] for c in range(3)]

    def bonds(p):
        everything = jnp.where(pair_ref[0, p] == pair_ref[1, p], 0, -1)
        live = jnp.where(p < count, -1, 0)
        return bits_ref[pl.ds(p, 8, stride=pairs), :] & (keep | everything) & live

    def advance(u, p, word, rounds):
        home = (pair_ref[0, p], pair_ref[0, p + 1])
        away = (pair_ref[1, p], pair_ref[1, p + 1])
        here = [spread(c, *home) for c in range(6)]
        table = [spread(c, *away) for c in range(6)]
        force = [jnp.zeros((8, 128), jnp.float32) for _ in range(3)]
        for _ in range(rounds):
            word, force = take_round(word, here, table, force)
        left_ref[u] = word
        for c in range(3):
            sums_refs[u][home[0] * 3 + c] += jnp.where(upper, force[c], 0.0)
            sums_refs[u][home[1] * 3 + c] += jnp.where(upper, 0.0, force[c])

    def step(q, carry):
        for u in range(GROUP // 2):
            p = q * GROUP + 2 * u
            advance(u, p, jnp.where(upper, bonds(p), bonds(p + 1)), STEADY)

        def more(r, carry):
            for u in range(GROUP // 2):
                advance(u, q * GROUP + 2 * u, left_ref[u], 1)
            return carry

        lax.fori_loop(STEADY, rounds_ref[q, 0], more, 0)
        return carry

    lax.fori_loop(0, (count + GROUP - 1) // GROUP, step, 0)

    for c in range(3):
        rows = [
            jnp.sum(sum(sums_ref[h * 3 + c] for sums_ref in sums_refs), axis=0, keepdims=True)
            for h in range(8)
        ]
        acceleration = stiffness * jnp.concatenate(rows, axis=0)
        acc_ref[c] = acceleration
        vel_ref[c] = vel_ref[c] + half_step * acceleration


SMEM = pl.BlockSpec(memory_space=pltpu.SMEM)
VMEM = pl.BlockSpec(memory_space=pltpu.VMEM)


LITTLE = pltpu.CompilerParams(vmem_limit_bytes=8 * 1024 * 1024)


def near(value):
    return pltpu.with_memory_space_constraint(value, pltpu.VMEM)


def aside(value):
    return pltpu.with_memory_space_constraint(value, pltpu.HBM)


def call_pack(owner, myself, fields):
    return pl.pallas_call(
        pack_kernel,
        out_shape=pltpu.VMEM((PACK, 128), jnp.float32),
        in_specs=[SMEM, SMEM] + [VMEM] * 4,
        out_specs=VMEM,
        compiler_params=LITTLE,
        name="pack",
    )(aside(owner), myself, *(aside(field) for field in fields))


def call_settle(owner, myself, fields, candidates, lattice):
    return pl.pallas_call(
        settle_kernel,
        out_shape=(
            pltpu.VMEM((CELL, 128), jnp.float32),
            pltpu.VMEM((lattice, 128), jnp.float32),
        ),
        in_specs=[SMEM, SMEM] + [VMEM] * 5,
        out_specs=(VMEM, VMEM),
        compiler_params=LITTLE,
        name="settle",
    )(owner, myself, *fields, near(candidates))


def call_force(pair_blocks, pair_count, sources, around, tops, wide, rounds):
    keep = jnp.asarray(self_bits())
    tile = jax.ShapeDtypeStruct((3, 8, 128), jnp.float32)
    return pl.pallas_call(
        force_kernel,
        out_shape=(tile, tile, tile),
        in_specs=[SMEM] * 4 + [VMEM] * 4,
        out_specs=(VMEM, VMEM, VMEM),
        scratch_shapes=[
            pltpu.VMEM((COMPS * 24, 128), jnp.float32),
            pltpu.VMEM((6 * 32, 128), jnp.float32),
            pltpu.VMEM((GROUP // 2, 8, 128), jnp.int32),
        ]
        + [pltpu.VMEM((24, 8, 128), jnp.float32)] * 4,
        compiler_params=LITTLE,
        name="forces",
    )(
        pair_blocks,
        pair_count,
        sources,
        rounds,
        near(around),
        near(tops),
        near(wide),
        keep,
    )


def shifted_by(shard, axis, amount):
    size = lax.axis_size(axis)
    return lax.ppermute(shard, axis, [(i, (i + amount) % size) for i in range(size)])


def around_index(offset, extent):
    wrapped = offset % extent
    return jnp.where(wrapped == 0, 1, jnp.where(wrapped == 1, 2, 0))


def per_device(
    ref_pos,
    displace,
    velocity,
    acceleration,
    new_owner,
    ghost_ids,
    pair_blocks,
    pair_count,
    bond_bits,
):
    blocks = ref_pos.shape[0]
    size_x, size_y, size_z = (lax.axis_size(axis) for axis in AXES)
    place_x, place_y, place_z = (lax.axis_index(axis) for axis in AXES)
    myself = ((place_x * size_y + place_y) * size_z + place_z).astype(jnp.int32)
    fields = tuple(
        jnp.transpose(field, (1, 0, 2)) for field in (ref_pos, displace, velocity, acceleration)
    )

    body = call_pack(new_owner, myself[None], fields)
    for axis in AXES:
        before = shifted_by(body, axis, 1)
        after = shifted_by(body, axis, -1)
        body = jnp.concatenate([before, body, after], axis=0)
    around, top = call_settle(
        new_owner, myself[None], fields, body, lax.axis_size(LATTICE)
    )
    tops = lax.all_to_all(top, LATTICE, 0, 0, tiled=True)

    ghost_dev = ghost_ids // blocks
    ghost_slot = ghost_ids % blocks
    sources = (
        around_index(ghost_dev // (size_y * size_z) - place_x, size_x)
        + around_index(ghost_dev // size_z % size_y - place_y, size_y) * 3
        + around_index(ghost_dev % size_z - place_z, size_z) * 9
    ) * CELL + ghost_slot
    sources = sources.astype(jnp.int32)
    for axis in AXES:
        before = shifted_by(around, axis, 1)
        after = shifted_by(around, axis, -1)
        around = jnp.concatenate([before, around, after], axis=0)
    wide, rounds = call_prepare(bond_bits)
    outs = call_force(pair_blocks, pair_count, sources, around, tops, wide, rounds)
    return tuple(jnp.transpose(out, (1, 0, 2)) for out in outs)


def solution(mesh):
    sizes = [mesh.shape[axis] for axis in ("gx", "gy", "gz")]
    split = Mesh(mesh.devices.reshape([n for size in sizes for n in (size // 2, 2)]), ALL)
    wide = P(ALL, None, None)
    in_specs = (wide,) * 4 + (P(ALL), P(ALL), P(None, ALL), P(ALL), wide)

    return jax.shard_map(
        per_device, mesh=split, in_specs=in_specs, out_specs=(wide,) * 3, check_vma=False
    )
```

```python
import functools

import jax
import jax.numpy as jnp
import numpy as np
from jax import lax
from jax.experimental import pallas as pl
from jax.experimental.pallas import tpu as pltpu
from jax.sharding import Mesh
from jax.sharding import PartitionSpec as P

WORD_BITS = 11
GX = ("gx_half", "gx_odd")
GY = ("gy_half", "gy_odd")
GZ = ("gz_half", "gz_odd")
AXES = (GX, GY, GZ)
ALL = GX + GY + GZ
LATTICE = ("gx_half", "gy_half", "gz_half")

courant = 0.05
stiffness = 20.0


COMPS = 12
PACK = 32
CELL = 96
ROWS = 8
GROUP = 24
STEADY = 4
SUMS = 6


LANE_GATHER = lax.GatherDimensionNumbers(
    offset_dims=(),
    collapsed_slice_dims=(1,),
    start_index_map=(1,),
    operand_batching_dims=(0,),
    start_indices_batching_dims=(0,),
)


def by_lane(table, particle):
    return lax.gather(
        table,
        particle[:, :, None],
        LANE_GATHER,
        slice_sizes=(1, 1),
        mode=lax.GatherScatterMode.PROMISE_IN_BOUNDS,
    )


def prepare_kernel(words_ref, wide_ref, most_ref):
    pairs = words_ref.shape[1]

    def group(g, carry):
        start = pl.multiple_of(g * ROWS, ROWS)
        words = [words_ref[w, pl.ds(start, ROWS), :] for w in range(12)]
        most = None
        for t in range(4):
            total = None
            for w in range(12):
                move = WORD_BITS * w - 32 * t
                if -WORD_BITS < move < 32:
                    part = words[w] << move if move >= 0 else words[w] >> -move
                    total = part if total is None else total | part
            wide_ref[t, pl.ds(start, ROWS), :] = total
            wide_ref[4 + t, pl.ds(start, ROWS), :] = total
            used = lax.population_count(total)
            most = used if most is None else jnp.maximum(most, used)
        most_ref[pl.ds(g, 1), :] = jnp.max(most, axis=0, keepdims=True)
        return carry

    lax.fori_loop(0, pairs // ROWS, group, 0, unroll=3)
    most_ref[...] = jnp.broadcast_to(
        jnp.max(most_ref[...], axis=1, keepdims=True), most_ref.shape
    )


def call_prepare(bond_bits):
    pairs = bond_bits.shape[0]
    wide, most = pl.pallas_call(
        prepare_kernel,
        out_shape=(
            pltpu.VMEM((8, pairs, 128), jnp.int32),
            jax.ShapeDtypeStruct((pairs // ROWS, 128), jnp.int32),
        ),
        in_specs=[VMEM],
        out_specs=(VMEM, VMEM),
        cost_estimate=pl.CostEstimate(
            flops=20_000_000, bytes_accessed=2_200_000, transcendentals=0
        ),
        compiler_params=LITTLE,
        name="prepare",
    )(jnp.transpose(bond_bits, (1, 0, 2)))
    return wide.reshape(8 * pairs, 128), most


def self_bits():
    bit = np.arange(128)[None, :] - 32 * (np.arange(8)[:, None] % 4)
    lost = np.where((bit >= 0) & (bit < 32), np.int64(1) << np.clip(bit, 0, 31), 0)
    return (~lost).astype(np.uint32).view(np.int32)


def pack_kernel(owner_ref, self_ref, ref_ref, dis_ref, vel_ref, acc_ref, out_ref):
    myself = self_ref[0]
    first = jnp.int32(0)
    second = jnp.int32(0)
    found = jnp.bool_(False)
    for k in range(8):
        leaves = owner_ref[k] != myself
        first = jnp.where(leaves & jnp.logical_not(found), k, first)
        second = jnp.where(leaves & found, k, second)
        found = found | leaves
    for group, source in enumerate((ref_ref, dis_ref, vel_ref, acc_ref)):
        for c in range(3):
            out_ref[pl.ds(group * 3 + c, 1), :] = source[c, pl.ds(first, 1), :]
            out_ref[pl.ds(12 + group * 3 + c, 1), :] = source[c, pl.ds(second, 1), :]
    lane = lax.broadcasted_iota(jnp.int32, (8, 128), 1)
    values = (
        owner_ref[first],
        owner_ref[second],
        myself * 8 + first,
        myself * 8 + second,
    )
    misc = jnp.zeros((8, 128), jnp.float32)
    for place, value in enumerate(values):
        misc = jnp.where(lane == place, value.astype(jnp.float32), misc)
    row = lax.broadcasted_iota(jnp.int32, (8, 128), 0)
    speed = jnp.maximum(
        jnp.maximum(jnp.abs(vel_ref[0]), jnp.abs(vel_ref[1])), jnp.abs(vel_ref[2])
    )
    out_ref[24:32, :] = jnp.where(row == 0, misc, jnp.max(speed))


def settle_kernel(
    owner_ref, self_ref, ref_ref, dis_ref, vel_ref, acc_ref, cand_ref, out_ref, top_ref
):
    myself = self_ref[0]
    misc = cand_ref[pl.ds(24, 27, stride=PACK), :]
    lane = lax.broadcasted_iota(jnp.int32, misc.shape, 1)
    place = lax.broadcasted_iota(jnp.int32, misc.shape, 0) * 2 + lane
    labels = pltpu.roll(misc, 126, 1)
    mine = (lane < 2) & (misc == myself.astype(jnp.float32))
    none = 1e9
    keys = jnp.where(mine, labels * 64.0 + place.astype(jnp.float32), none)
    first_key = jnp.min(keys)
    first = first_key.astype(jnp.int32)
    second = jnp.min(jnp.where(keys > first_key, keys, none)).astype(jnp.int32)
    lower = (first >> 6 < myself * 8).astype(jnp.int32) + (second >> 6 < myself * 8).astype(
        jnp.int32
    )
    spots = (jnp.where(lower >= 1, 0, 6), jnp.where(lower == 2, 1, 7))
    sources = (ref_ref, dis_ref, vel_ref, acc_ref)
    slot = lower
    for k in range(8):
        stays = owner_ref[k] == myself
        target = jnp.where(stays, slot, spots[0])
        slot = slot + stays.astype(jnp.int32)
        for row in range(COMPS):
            out_ref[pl.ds(row * 8 + target, 1), :] = sources[row // 3][row % 3, k : k + 1, :]
    for key, spot in zip((first, second), spots):
        base = ((key & 63) >> 1) * PACK + (key & 1) * COMPS
        for row in range(COMPS):
            out_ref[pl.ds(row * 8 + spot, 1), :] = cand_ref[pl.ds(base + row, 1), :]
    tops = cand_ref[pl.ds(25, 27, stride=PACK), :]
    top_ref[...] = jnp.broadcast_to(jnp.max(tops, axis=0, keepdims=True), top_ref.shape)


def whole(number, divisor):
    power = divisor.bit_length() - 1
    return number >> power if divisor == 1 << power else lax.div(number, divisor)


def rest(number, divisor):
    return number & (divisor - 1) if divisor & (divisor - 1) == 0 else lax.rem(number, divisor)


def grid_place(device, sizes):
    return (
        whole(device, sizes[1] * sizes[2]),
        rest(whole(device, sizes[2]), sizes[1]),
        rest(device, sizes[2]),
    )


def around_index(offset, place, extent):
    wrapped = rest(offset + extent, extent)
    ahead = (wrapped == 1) == ((place & 1) == 0)
    return jnp.where(wrapped == 0, 1, jnp.where(ahead, 2, 0))


def force_kernel(
    sizes,
    pair_ref,
    count_ref,
    ghost_ref,
    self_ref,
    rounds_ref,
    around_ref,
    tops_ref,
    bits_ref,
    keep_ref,
    dis_ref,
    vel_ref,
    acc_ref,
    raw_ref,
    ext_ref,
    left_ref,
    *sums_refs,
):
    pairs = pair_ref.shape[1]
    fastest = jnp.broadcast_to(jnp.max(tops_ref[...], axis=0, keepdims=True), (8, 128))
    timestep = courant / (fastest + 1e-06)
    half_step = 0.5 * timestep

    def own(c):
        start = 13 * CELL + 8 * c
        return around_ref[start : start + 8, :]

    for c in range(3):
        halfway = own(6 + c) + half_step * own(9 + c)
        shifted = own(3 + c) + timestep * halfway
        dis_ref[c] = shifted
        vel_ref[c] = halfway
        ext_ref[c * 32 : c * 32 + 8, :] = own(c)
        ext_ref[(3 + c) * 32 : (3 + c) * 32 + 8, :] = shifted

    myself = grid_place(self_ref[0], sizes)
    for g in range(24):
        block = ghost_ref[g]
        owner = grid_place(block >> 3, sizes)
        cells = [around_index(o - m, m, n) for o, m, n in zip(owner, myself, sizes)]
        start = (cells[0] + 3 * cells[1] + 9 * cells[2]) * CELL + (block & 7)
        for c in range(COMPS):
            raw_ref[c * 24 + g : c * 24 + g + 1, :] = around_ref[pl.ds(start + 8 * c, 1), :]

    for c in range(3):
        for t in range(3):

            def raw(n):
                return raw_ref[n * 24 + t * 8 : n * 24 + t * 8 + 8, :]

            halfway = raw(6 + c) + half_step * raw(9 + c)
            row = 8 + t * 8
            ext_ref[c * 32 + row : c * 32 + row + 8, :] = raw(c)
            ext_ref[(3 + c) * 32 + row : (3 + c) * 32 + row + 8, :] = raw(3 + c) + timestep * halfway

    for k in range(24):
        for sums_ref in sums_refs:
            sums_ref[k] = jnp.zeros((8, 128), jnp.float32)

    count = count_ref[0]
    keep = keep_ref[...]
    row = lax.broadcasted_iota(jnp.int32, (8, 128), 0)
    upper = row < 4
    first = (row & 3) * 32

    def spread(c, one, other):
        return jnp.where(
            upper,
            jnp.broadcast_to(ext_ref[pl.ds(c * 32 + one, 1), :], (8, 128)),
            jnp.broadcast_to(ext_ref[pl.ds(c * 32 + other, 1), :], (8, 128)),
        )

    def take_round(word, here, table, force):
        below = word - 1
        particle = (lax.population_count(below & ~word) + first) & 127
        there = [by_lane(table[c], particle) for c in range(6)]
        gap = [there[c] - here[c] for c in range(3)]
        now = [gap[c] + (there[3 + c] - here[3 + c]) for c in range(3)]
        rest2 = gap[0] * gap[0] + gap[1] * gap[1] + gap[2] * gap[2]
        now2 = now[0] * now[0] + now[1] * now[1] + now[2] * now[2]
        scaled = lax.rsqrt(rest2) - lax.rsqrt(now2)
        scaled = jnp.where(word != 0, scaled, 0.0)
        return word & below, [force[c] + scaled * now[c] for c in range(3)]

    def bonds(p):
        everything = jnp.where(pair_ref[0, p] == pair_ref[1, p], 0, -1)
        live = jnp.where(p < count, -1, 0)
        return bits_ref[pl.ds(p, 8, stride=pairs), :] & (keep | everything) & live

    def advance(u, p, word, rounds):
        home = (pair_ref[0, p], pair_ref[0, p + 1])
        away = (pair_ref[1, p], pair_ref[1, p + 1])
        here = [spread(c, *home) for c in range(6)]
        table = [spread(c, *away) for c in range(6)]
        force = [jnp.zeros((8, 128), jnp.float32) for _ in range(3)]
        for _ in range(rounds):
            word, force = take_round(word, here, table, force)
        left_ref[u] = word
        for c in range(3):
            sums_refs[u % SUMS][home[0] * 3 + c] += jnp.where(upper, force[c], 0.0)
            sums_refs[u % SUMS][home[1] * 3 + c] += jnp.where(upper, 0.0, force[c])

    def step(q, carry):
        for u in range(GROUP // 2):
            p = q * GROUP + 2 * u
            advance(u, p, jnp.where(upper, bonds(p), bonds(p + 1)), STEADY)

        def more(r, carry):
            for u in range(GROUP // 2):
                advance(u, q * GROUP + 2 * u, left_ref[u], 1)
            return carry

        rounds = rounds_ref[q * (GROUP // ROWS), 0]
        for n in range(1, GROUP // ROWS):
            rounds = jnp.maximum(rounds, rounds_ref[q * (GROUP // ROWS) + n, 0])
        lax.fori_loop(STEADY, rounds, more, 0)
        return carry

    lax.fori_loop(0, (count + GROUP - 1) // GROUP, step, 0)

    for c in range(3):
        rows = [
            jnp.sum(sum(sums_ref[h * 3 + c] for sums_ref in sums_refs), axis=0, keepdims=True)
            for h in range(8)
        ]
        acceleration = stiffness * jnp.concatenate(rows, axis=0)
        acc_ref[c] = acceleration
        vel_ref[c] = vel_ref[c] + half_step * acceleration


SMEM = pl.BlockSpec(memory_space=pltpu.SMEM)
VMEM = pl.BlockSpec(memory_space=pltpu.VMEM)


LITTLE = pltpu.CompilerParams(vmem_limit_bytes=8 * 1024 * 1024)


def near(value):
    return pltpu.with_memory_space_constraint(value, pltpu.VMEM)


def aside(value):
    return pltpu.with_memory_space_constraint(value, pltpu.HBM)


def call_pack(owner, myself, fields):
    return pl.pallas_call(
        pack_kernel,
        out_shape=pltpu.VMEM((PACK, 128), jnp.float32),
        in_specs=[SMEM, SMEM] + [VMEM] * 4,
        out_specs=VMEM,
        compiler_params=LITTLE,
        name="pack",
    )(aside(owner), myself, *(aside(field) for field in fields))


def call_settle(owner, myself, fields, candidates, lattice):
    return pl.pallas_call(
        settle_kernel,
        out_shape=(
            pltpu.VMEM((CELL, 128), jnp.float32),
            pltpu.VMEM((lattice, 128), jnp.float32),
        ),
        in_specs=[SMEM, SMEM] + [VMEM] * 5,
        out_specs=(VMEM, VMEM),
        compiler_params=LITTLE,
        name="settle",
    )(owner, myself, *fields, near(candidates))


def call_force(sizes, pair_blocks, pair_count, ghost_ids, myself, around, tops, wide, rounds):
    keep = jnp.asarray(self_bits())
    tile = jax.ShapeDtypeStruct((3, 8, 128), jnp.float32)
    return pl.pallas_call(
        functools.partial(force_kernel, sizes),
        out_shape=(tile, tile, tile),
        in_specs=[SMEM] * 5 + [VMEM] * 4,
        out_specs=(VMEM, VMEM, VMEM),
        scratch_shapes=[
            pltpu.VMEM((COMPS * 24, 128), jnp.float32),
            pltpu.VMEM((6 * 32, 128), jnp.float32),
            pltpu.VMEM((GROUP // 2, 8, 128), jnp.int32),
        ]
        + [pltpu.VMEM((24, 8, 128), jnp.float32)] * SUMS,
        compiler_params=LITTLE,
        name="forces",
    )(
        pair_blocks,
        pair_count,
        ghost_ids,
        myself,
        rounds,
        near(around),
        near(tops),
        near(wide),
        keep,
    )


def swapped(shard, axis, odd):
    size = lax.axis_size(axis)
    return lax.ppermute(
        shard, axis, [(i, (i + 1 if i % 2 == odd else i - 1) % size) for i in range(size)]
    )


def per_device(
    ref_pos,
    displace,
    velocity,
    acceleration,
    new_owner,
    ghost_ids,
    pair_blocks,
    pair_count,
    bond_bits,
):
    sizes = tuple(lax.axis_size(axis) for axis in AXES)
    place_x, place_y, place_z = (lax.axis_index(axis) for axis in AXES)
    myself = ((place_x * sizes[1] + place_y) * sizes[2] + place_z).astype(jnp.int32)
    fields = tuple(
        jnp.transpose(field, (1, 0, 2)) for field in (ref_pos, displace, velocity, acceleration)
    )

    body = call_pack(new_owner, myself[None], fields)
    for axis in AXES:
        before = swapped(body, axis, 1)
        after = swapped(body, axis, 0)
        body = jnp.concatenate([before, body, after], axis=0)
    around, top = call_settle(
        new_owner, myself[None], fields, body, lax.axis_size(LATTICE)
    )
    tops = lax.all_to_all(top, LATTICE, 0, 0, tiled=True)

    for axis in AXES:
        before = swapped(around, axis, 1)
        after = swapped(around, axis, 0)
        around = jnp.concatenate([before, around, after], axis=0)
    wide, rounds = call_prepare(bond_bits)
    outs = call_force(
        sizes, pair_blocks, pair_count, ghost_ids, myself[None], around, tops, wide, rounds)
    return tuple(jnp.transpose(out, (1, 0, 2)) for out in outs)


def solution(mesh):
    sizes = [mesh.shape[axis] for axis in ("gx", "gy", "gz")]
    split = Mesh(mesh.devices.reshape([n for size in sizes for n in (size // 2, 2)]), ALL)
    wide = P(ALL, None, None)
    in_specs = (wide,) * 4 + (P(ALL), P(ALL), P(None, ALL), P(ALL), wide)

    return jax.shard_map(
        per_device, mesh=split, in_specs=in_specs, out_specs=(wide,) * 3, check_vma=False
    )
```
